256 devices in a mesh: row: 8 (over y, core), col: 32 (over x, z).
Axes of the slice: x: 4, y: 4, z: 8, core: 2. Of those that a mesh axis runs over, the one named last changes fastest.
Arguments:
- weights: float32 [40, 2048, 4096], P(None, 'row', 'col'), may hold values from -0.006214806 to 0.006214806
- pool: float32 [12, 2048, 4096], P(None, 'row', 'col'), may hold values from -6 to 6
- desired: float32 [12, 8], replicated, may hold values from -6 to 6
- plan: int32 [2, 16], replicated, may hold values from 0 to 11
- beam_ref: int32 [40], replicated, may hold values from 0 to 7
- step_size: float32 [40], replicated, may hold values from 0.2 to 0.8
- smoothing: float32 [40], replicated, may hold values from 0.05 to 0.2
- active: int32 [40], replicated, may hold values from 1 to 2
Outputs:
- final_weights: float32 [40, 2048, 4096], P(None, 'row', 'col')
- errors: float32 [2, 40, 16], replicated
The draws below stay inside these ranges and needn't reach their ends.
Inputs may be any that keep to these rules, and one draw needn't show every extreme that they name: `plan`: indices of recorded snapshots. `beam_ref`: indices of reference signals.
All inputs are finite; a program needn't handle non-finite values.
Results may differ from the reference program's by a relative error of at most 0.00017.
Values sent between devices are 32-bit elements; how exact they have to be, the bound alone decides.
No kernel may reach another device: no remote copies, remote signals or barrier semaphores. Data moves between devices by JAX's collectives and lax.ppermute only.
A program may use at most 128 MiB of HBM per device.

```python
import math
import jax
import jax.numpy as jnp
from jax import lax

NR = 2048
NC = 4096
B = 40
S = 16
POOL = 12
REFS = 8
ITERS = 2


def set_ends(values, stream_key, least, high):
    longest = values.shape.index(max(values.shape))
    spots = []
    for shift in (0, 1):
        where = [jax.random.randint(jax.random.fold_in(stream_key, axis), (), 0, length) for axis, length in enumerate(values.shape)]
        where[longest] = (where[longest] + shift) % values.shape[longest]
        spots.append(tuple(where))
    return values.at[spots[0]].set(least).at[spots[1]].set(high)


def levels(own_key, extent, pieces, least, top_value):
    factor_of = 1.0
    for dim, parts in pieces:
        draws = jax.random.uniform(jax.random.fold_in(jax.random.fold_in(own_key, 6), dim), (parts,), jnp.float32, least / len(pieces), top_value / len(pieces))
        factor_of = factor_of * jnp.repeat(jnp.exp(draws), extent[dim] // parts).reshape((-1,) + (1,) * (len(extent) - 1 - dim))
    return factor_of


def noise(stream_key, shape, width, bound, cuts=(), dtype=jnp.bfloat16):
    values = width * jax.random.normal(stream_key, shape, jnp.float32)
    if cuts:
        values = values * levels(stream_key, shape, cuts, -0.22, 0.18)
    return jnp.clip(values, -bound, bound).astype(dtype)


def setup_inputs(seed: int = 0) -> dict:
    key_of = jax.random.split(jax.random.key(seed), 9)
    weights = noise(key_of[0], (B, NR, NC), (3.0 / (NR * NC) ** 0.5), 0.006214806, ((1, 8), (2, 32)), jnp.float32)
    pool = noise(key_of[1], (POOL, NR, NC), 1.0, 6.0, ((1, 8), (2, 32)), jnp.float32)
    desired = noise(key_of[2], (POOL, REFS), 1.0, 6.0, (), jnp.float32)
    plan = set_ends(jax.random.randint(key_of[3], (ITERS, S), 0, POOL), jax.random.fold_in(key_of[3], 1), 0, POOL - 1).astype(jnp.int32)
    beam_ref = set_ends(jax.random.randint(key_of[4], (B,), 0, REFS), jax.random.fold_in(key_of[4], 1), 0, REFS - 1).astype(jnp.int32)
    step_size = jnp.clip(jnp.exp(jax.random.uniform(key_of[5], (B,), jnp.float32, math.log(0.2), math.log(0.8))), 0.2, 0.8)
    smoothing = jnp.clip(jax.random.uniform(key_of[6], (B,), jnp.float32, 0.05, 0.2), 0.05, 0.2)
    active = set_ends(jax.random.randint(key_of[7], (B,), 1, ITERS + 1), jax.random.fold_in(key_of[7], 1), 1, ITERS).astype(jnp.int32)
    return {"weights": weights, "pool": pool, "desired": desired, "plan": plan, "beam_ref": beam_ref, "step_size": step_size, "smoothing": smoothing, "active": active}


def laplace(field):
    padded = jnp.pad(field, ((0, 0), (1, 1), (1, 1)))
    return padded[:, 2:, 1:-1] + padded[:, :-2, 1:-1] + padded[:, 1:-1, 2:] + padded[:, 1:-1, :-2] - 4.0 * field

def reference(weights, pool, desired, plan, beam_ref, step_size, smoothing, active):
    scale = 1.0 / math.sqrt(NR * NC)
    current = weights
    history = []
    for step in range(ITERS):
        snaps = jnp.take(pool, plan[step], axis=0).reshape(S, -1)
        beam_out = jnp.dot(current.reshape(B, -1), snaps.T, precision=lax.Precision.HIGHEST) * scale
        target = jnp.take(desired, plan[step], axis=0)[:, beam_ref].T
        error = target - beam_out
        history.append(error)
        grad = jnp.dot(error, snaps, precision=lax.Precision.HIGHEST).reshape(current.shape)
        live = (active > step).astype(jnp.float32)[:, None, None]
        update = step_size[:, None, None] * scale * grad + smoothing[:, None, None] * laplace(current)
        current = current + live * update
    return (current, jnp.stack(history))
```

```python
import math

import jax
import jax.numpy as jnp
from jax import lax
from jax.experimental import pallas as pl
from jax.experimental.pallas import tpu as pltpu
from jax.sharding import Mesh
from jax.sharding import PartitionSpec as P

NR = 2048
NC = 4096
ROW = ("row_0", "row_1")
COL = ("col_0", "col_1")
NEAR = ("row_1", "col_1")
FAR = ("row_0", "col_0")
SCALE = 1.0 / math.sqrt(NR * NC)
BEAMS, POOL, ROWS, LANES = 40, 12, 256, 128
GROUP = 4
LIMIT = 30 << 20
EXACT = lax.Precision.HIGHEST
NN = (((1,), (0,)), ((), ()))
NT = (((1,), (1,)), ((), ()))
TN = (((0,), (0,)), ((), ()))
F32, BF16 = jnp.float32, jnp.bfloat16
VMEM = pl.BlockSpec(memory_space=pltpu.VMEM)
HBM = pl.BlockSpec(memory_space=pltpu.HBM)
SMEM = pl.BlockSpec(memory_space=pltpu.SMEM)


def iota(shape, dim):
    return lax.broadcasted_iota(jnp.int32, shape, dim)


def dot(a, b, dims, precision=None):
    return lax.dot_general(a, b, dims, precision=precision, preferred_element_type=F32)


def halves(x):
    high = x.astype(BF16)
    return high, (x - high.astype(F32)).astype(BF16)


def thirds(x):
    high = x.astype(BF16)
    rest = x - high.astype(F32)
    mid = rest.astype(BF16)
    return high, mid, (rest - mid.astype(F32)).astype(BF16)


def dot_exact(ones, x, dims):
    return sum(dot(ones.astype(BF16), part, dims) for part in thirds(x))


def exact_dot(x, ones, dims):
    return sum(dot(part, ones.astype(BF16), dims) for part in thirds(x))


def rows_around(x):
    zero = jnp.zeros((1, LANES), F32)
    return jnp.concatenate([x[1:], zero], axis=0) + jnp.concatenate([zero, x[:-1]], axis=0)


def band_matrix(center):
    away = jnp.abs(iota((LANES, LANES), 0) - iota((LANES, LANES), 1))
    return jnp.where(away == 0, center, jnp.where(away == 1, 1.0, 0.0))


def lap_inside(x, along):
    return rows_around(x) + dot(jnp.concatenate(halves(x), axis=1), along, NN)


def line_ends(w_hbm, pool_hbm, top_ref, bottom_ref, w_buf, pool_buf, sems):
    copies = []
    for k, at in enumerate((0, ROWS - 8)):
        for j, (src, dst) in enumerate(((w_hbm, w_buf), (pool_hbm, pool_buf))):
            copies.append(pltpu.make_async_copy(src.at[:, at : at + 8, :], dst.at[k], sems.at[2 * k + j]))
    for copy in copies:
        copy.start()
    for copy in copies:
        copy.wait()
    for k, (ref, near, far) in enumerate(((top_ref, 0, 1), (bottom_ref, 7, 6))):
        ref[0:40, :] = w_buf[k, :, near, :]
        ref[40:80, :] = w_buf[k, :, far, :]
        ref[80:96, :] = jnp.zeros((16, LANES), F32)
        ref[80:92, :] = pool_buf[k, :, near, :]


def column_ends(w_hbm, pool_hbm, left_ref, right_ref, w_buf, pool_buf, ends_ref, sems):
    copies = [pltpu.make_async_copy(pool_hbm, pool_buf, sems.at[5])]
    for k in range(5):
        copies.append(pltpu.make_async_copy(w_hbm.at[8 * k : 8 * k + 8], w_buf.at[8 * k : 8 * k + 8], sems.at[k]))
    for copy in copies:
        copy.start()
    row, lane = iota((8, LANES), 0), iota((8, LANES), 1)
    pick = jnp.zeros((8, LANES), F32)
    for k, spot in enumerate((0, LANES - 1, 1, LANES - 2)):
        pick = jnp.where((row == k) & (lane == spot), 1.0, pick)
    pick = pick.astype(BF16)
    pick = jnp.concatenate([pick, pick], axis=1)

    def taken(ref, first):
        def image(p, carry):
            ends_ref[first + p] = dot(pick, jnp.concatenate(halves(ref[p]), axis=1), NT)
            return carry

        return image

    copies[0].wait()
    lax.fori_loop(0, POOL, taken(pool_buf, BEAMS), 0, unroll=4)
    for k in range(5):
        copies[1 + k].wait()
        lax.fori_loop(8 * k, 8 * k + 8, taken(w_buf, 0), 0, unroll=4)
    for ref, near, far in ((left_ref, 0, 2), (right_ref, 1, 3)):
        ref[0:40, :] = ends_ref[0:40, near, :]
        ref[40:80, :] = ends_ref[0:40, far, :]
        ref[80:96, :] = jnp.zeros((16, ROWS), F32)
        ref[80:92, :] = ends_ref[40:52, near, :]


def gram(w_ref, pool_ref, sums_ref, lap_ref, acc_ref):
    along = band_matrix(-4.0).astype(BF16)
    along = jnp.concatenate([along, along], axis=0)
    acc_ref[...] = jnp.zeros_like(acc_ref)

    def smooth(p, carry):
        lap_ref[p] = lap_inside(pool_ref[p], along)
        return carry

    lax.fori_loop(0, POOL, smooth, 0, unroll=4)

    def pair(ref, count, t):
        parts = []
        for k in range(GROUP):
            at = pl.multiple_of(t * GROUP * 8 + k * 8, 8)
            parts.append(ref[:, pl.ds(at, 8), :].reshape(count * 8, LANES))
        return jnp.concatenate(parts, axis=1)

    def step(t, carry):
        p_high, p_low = halves(pair(pool_ref, POOL, t))
        l_high, l_low = halves(pair(lap_ref, POOL, t))
        w_high, w_low = halves(pair(w_ref, BEAMS, t))
        a_high = jnp.concatenate([w_high, p_high], axis=0)
        a_low = jnp.concatenate([w_low, p_low], axis=0)
        b_high = jnp.concatenate([p_high, l_high], axis=0)
        b_low = jnp.concatenate([p_low, l_low], axis=0)
        left = jnp.concatenate([a_high, a_high, a_low], axis=1)
        right = jnp.concatenate([b_high, b_low, b_high], axis=1)
        acc_ref[...] += dot(left, right, NT)
        return carry

    lax.fori_loop(0, 32 // GROUP, step, 0)
    n, m = acc_ref.shape
    same = (iota((n, m), 0) & 7) == (iota((n, m), 1) & 7)
    kept = jnp.where(same, acc_ref[...], 0.0)
    q, j = iota((32, m), 0), iota((32, m), 1) >> 3
    fold = jnp.where(((j < POOL) & (q == j)) | ((j >= POOL) & (q == j + 16 - POOL)), 1.0, 0.0)
    folded = dot_exact(fold, kept, NT)
    i, lane = iota((n, LANES), 0) >> 3, iota((n, LANES), 1)
    to_p = jnp.where(((i < BEAMS) & (lane == i)) | ((i >= BEAMS) & (lane == i + 80 - BEAMS)), 1.0, 0.0)
    to_l = jnp.where((i < BEAMS) & (lane == i + 40), 1.0, 0.0)
    sums = exact_dot(folded[0:16], to_p, NN) + exact_dot(folded[16:32], to_l, NN)
    sums_ref[...] = sums[0:POOL]


def again(parts_ref, out_ref):
    sums = parts_ref[0]
    for k in range(1, 16):
        sums = sums + parts_ref[k]
    for k in range(16):
        out_ref[k] = sums


def base(
    smooth_ref, active_ref, w_ref, pool_lap_ref, sums_ref, smooth_row_ref, active_row_ref,
    top_ref, bottom_ref, left_ref, right_ref, up_ref, down_ref, west_ref, east_ref,
    sent_ref, out_ref, lap_ref, fix_ref, p_fix_ref,
):
    halo = jnp.concatenate([ref[80:96, :] for ref in (west_ref, east_ref, up_ref, down_ref)], axis=1)
    edge = jnp.concatenate([ref[0:40, :] for ref in (left_ref, right_ref, top_ref, bottom_ref)], axis=1)
    edge = jnp.concatenate([jnp.zeros((40, 768), F32), edge, jnp.zeros((48, 768), F32)], axis=0)
    sums = sums_ref[...] + dot(halo, edge, NT, EXACT)[0:POOL]
    for k in range(16):
        sent_ref[k] = sums

    def across(row):
        return jnp.broadcast_to(row, (8, BEAMS)).T[:, 0:1]

    smooth_row, active_row = smooth_row_ref[...], active_row_ref[...]
    live0 = jnp.where(active_row > 0, 1.0, 0.0)
    live1 = jnp.where(active_row > 1, 1.0, 0.0)
    a = across(smooth_row * (live0 + live1))
    c = across(smooth_row * smooth_row * live0 * live1)
    r = lax.axis_index(ROW[0]) * 2 + lax.axis_index(ROW[1])
    k = lax.axis_index(COL[0]) * 8 + lax.axis_index(COL[1])
    has_up, has_down = jnp.where(r > 0, 1.0, 0.0), jnp.where(r < 7, 1.0, 0.0)
    has_west, has_east = jnp.where(k > 0, 1.0, 0.0), jnp.where(k < 31, 1.0, 0.0)
    span, shifted, corner = slice(0, 40), slice(40, 80), slice(96, 136)
    wide, thin = iota((BEAMS, ROWS), 1), iota((BEAMS, LANES), 1)

    def mixed(near, far, own, prev, after):
        return a * near + c * (2.0 * (prev + after) - 8.0 * near + far + own), c * near

    def column(msg_ref, own_ref, has):
        near = msg_ref[span, :]
        prev = jnp.where(wide == 0, 0.0, pltpu.roll(near, 1, 1))
        after = jnp.where(wide == ROWS - 1, 0.0, pltpu.roll(near, ROWS - 1, 1))
        return mixed(near, msg_ref[shifted, :], has * own_ref[span, :], prev, after)

    def line(msg_ref, own_ref, has, at):
        near = msg_ref[span, :]
        west = pltpu.roll(west_ref[corner, at : at + LANES], 1, 1)
        east = pltpu.roll(east_ref[corner, at : at + LANES], LANES - 1, 1)
        prev = jnp.where(thin == 0, west, pltpu.roll(near, 1, 1))
        after = jnp.where(thin == LANES - 1, east, pltpu.roll(near, LANES - 1, 1))
        return mixed(near, msg_ref[shifted, :], has * own_ref[span, :], prev, after)

    fix_ref[...] = jnp.zeros_like(fix_ref)
    fix_ref[:, 0, 0:256], fix_ref[:, 1, 0:256] = column(west_ref, left_ref, has_west)
    fix_ref[:, 2, 0:256], fix_ref[:, 3, 0:256] = column(east_ref, right_ref, has_east)
    fix_ref[:, 0, 256:384], fix_ref[:, 1, 256:384] = line(up_ref, top_ref, has_up, 0)
    fix_ref[:, 7, 384:512], fix_ref[:, 6, 384:512] = line(down_ref, bottom_ref, has_down, LANES)

    row, lane = iota((16, LANES), 0) & 7, iota((16, LANES), 1)
    place = jnp.zeros((16, LANES), F32)
    for k, spot in enumerate((0, 1, LANES - 1, LANES - 2)):
        place = jnp.where((row == k) & (lane == spot), 1.0, place)
    place = place.astype(BF16)

    def placed(x):
        high, low = halves(x)
        both = jnp.concatenate([high.astype(F32), low.astype(F32)], axis=0)
        return dot(both.T.astype(BF16), place, NN)

    p_fix_ref[...] = jnp.zeros_like(p_fix_ref)
    p_fix_ref[:, 0, :] = west_ref[80:92, :]
    p_fix_ref[:, 2, :] = east_ref[80:92, :]

    def pool_step(p, carry):
        lap_ref[p] = pool_lap_ref[p] + placed(p_fix_ref[p])
        return carry

    lax.fori_loop(0, POOL, pool_step, 0, unroll=4)
    lap_ref[:, 0, :] += up_ref[80:92, :]
    lap_ref[:, ROWS - 1, :] += down_ref[80:92, :]

    once = band_matrix(-2.0)
    twice = dot(once, once, NN)
    along = jnp.concatenate([once, twice], axis=1).astype(BF16)
    along = jnp.concatenate([along, along], axis=0)

    def beam(b, carry):
        x = w_ref[b]
        s_b, n_b = smooth_ref[b], active_ref[b]
        live0, live1 = jnp.where(n_b > 0, 1.0, 0.0), jnp.where(n_b > 1, 1.0, 0.0)
        a_b, c_b = s_b * (live0 + live1), s_b * s_b * live0 * live1
        sides = dot(jnp.concatenate(halves(x), axis=1), along, NN)
        one, two = sides[:, :LANES], sides[:, LANES:]
        down = rows_around(x) - 2.0 * x
        inner = a_b * x + c_b * (down + 2.0 * one)
        out = (x + a_b * one + c_b * two) + (rows_around(inner) - 2.0 * inner) + placed(fix_ref[b, :, 0:256])
        out_ref[b, 8 : ROWS - 8, :] = out[8 : ROWS - 8]
        out_ref[b, 0:8, :] = out[0:8] + fix_ref[b, :, 256:384]
        out_ref[b, ROWS - 8 : ROWS, :] = out[ROWS - 8 :] + fix_ref[b, :, 384:512]
        return carry

    lax.fori_loop(0, BEAMS, beam, 0, unroll=2)


def finish(
    parts_ref, desired_ref, plan_ref, ref_ref, rate_ref, smooth_ref, active_ref, base_ref, pool_ref, lap_ref,
    out_hbm, err_ref, done_ref, high_ref, low_ref, sems,
):
    def store(t):
        at = pl.ds(pl.multiple_of(t * 32, 8), 32)
        return pltpu.make_async_copy(done_ref.at[:, at, :], out_hbm.at[:, at, :], sems.at[t])

    sums = parts_ref[0]
    for k in range(1, 16):
        sums = sums + parts_ref[k]
    one_hot = jnp.where(iota((8, BEAMS), 0) == ref_ref[...], 1.0, 0.0)
    target = dot(desired_ref[...], one_hot, TN, EXACT)
    rate, smooth = rate_ref[...] * SCALE, smooth_ref[...]
    live0 = jnp.where(active_ref[...] > 0, 1.0, 0.0)
    live1 = jnp.where(active_ref[...] > 1, 1.0, 0.0)
    hits = [jnp.where(iota((POOL, 16), 0) == plan_ref[t : t + 1, :], 1.0, 0.0) for t in range(2)]
    many = [jnp.sum(h, axis=1, keepdims=True) for h in hits]
    p0 = sums[:, 0:BEAMS]
    lap = pltpu.roll(sums, LANES - 40, 1)[:, 0:BEAMS]
    inner = pltpu.roll(sums, LANES - 80, 1)[:, 0:POOL]
    e0 = target - SCALE * p0
    c0 = many[0] * e0
    p1 = p0 + live0 * (rate * dot(inner, c0, NN, EXACT) + smooth * lap)
    e1 = target - SCALE * p1
    c1 = many[1] * e1
    for t, e in enumerate((e0, e1)):
        err_ref[t] = dot(hits[t], e, TN, EXACT)
    d0 = rate * (live0 * c0 + live1 * c1)
    d1 = live0 * live1 * rate * smooth * c0
    gap = jnp.zeros((4, BEAMS), F32)
    both = jnp.concatenate([d0, gap, d1, gap], axis=0)
    spread = jnp.where((iota((320, BEAMS), 0) >> 3) == iota((320, BEAMS), 1), 1.0, 0.0)
    by_q = dot(spread, both, NT, EXACT)
    q, j = iota((32, 192), 0), iota((32, 192), 1) >> 3
    fold = jnp.where(((j < POOL) & (q == j)) | ((j >= POOL) & (q == j + 16 - POOL)), 1.0, 0.0)
    wide = dot(by_q, fold, NN, EXACT)
    same = (iota(wide.shape, 0) & 7) == (iota(wide.shape, 1) & 7)
    high, low = halves(jnp.where(same, wide, 0.0))
    high_ref[...] = high
    low_ref[...] = low

    def step(t, carry):
        def tile(ref, at):
            return ref.at[:, pl.ds(pl.multiple_of(t * 32 + at, 8), 8), :]

        for k in range(2):
            halves_of = []
            for h in range(2):
                at = 16 * k + 8 * h
                halves_of.append(
                    jnp.concatenate([tile(ref, at)[...].reshape(96, LANES) for ref in (pool_ref, lap_ref)], axis=0)
                )
            high, low = halves(jnp.concatenate(halves_of, axis=1))
            got = dot(high_ref[...], high, NN) + dot(high_ref[...], low, NN) + dot(low_ref[...], high, NN)
            for h in range(2):
                part = got[:, h * LANES : (h + 1) * LANES].reshape(BEAMS, 8, LANES)
                at = 16 * k + 8 * h
                tile(done_ref, at)[...] = tile(base_ref, at)[...] + part
        store(t).start()
        return carry

    lax.fori_loop(0, 8, step, 0)
    for t in range(8):
        store(t).wait()


def call(kernel, outs, specs, scratch=(), out_specs=None):
    run = pl.pallas_call(
        kernel,
        name=kernel.__name__,
        out_shape=outs,
        in_specs=specs,
        out_specs=out_specs or [VMEM] * len(outs),
        scratch_shapes=scratch,
        compiler_params=pltpu.CompilerParams(vmem_limit_bytes=LIMIT),
    )
    homes = {id(VMEM): pltpu.VMEM, id(HBM): pltpu.HBM}

    def at_home(value, spec):
        return pltpu.with_memory_space_constraint(value, homes[id(spec)]) if id(spec) in homes else value

    return lambda *args: run(*[at_home(x, spec) for x, spec in zip(args, specs)])


def vmem(*dims):
    return pltpu.VMEM(dims, F32)


def far_out(*dims):
    return pltpu.HBM(dims, F32)


def moved(value, axes, ahead):
    count = lax.axis_size(axes)
    pairs = [(i, i + 1) for i in range(count - 1)]
    return lax.ppermute(value, axes, pairs if ahead else [(b, a) for a, b in pairs])


def exchange(value, axes):
    return lax.all_to_all(value, axes, split_axis=0, concat_axis=0, tiled=True)


def body(weights, pool, desired, plan, beam_ref, step_size, smoothing, active):
    DMA = pltpu.SemaphoreType.DMA
    top, bottom = call(
        line_ends,
        [vmem(96, LANES)] * 2,
        [HBM, HBM],
        [vmem(2, BEAMS, 8, LANES), vmem(2, POOL, 8, LANES), DMA((4,))],
    )(weights, pool)
    from_up = moved(bottom, ROW, True)
    from_down = moved(top, ROW, False)
    left, right, w_near, p_near = call(
        column_ends,
        [vmem(96, ROWS)] * 2 + [vmem(BEAMS, ROWS, LANES), vmem(POOL, ROWS, LANES)],
        [HBM, HBM],
        [vmem(BEAMS + POOL, 8, ROWS), DMA((6,))],
    )(weights, pool)
    corners = jnp.concatenate([from_up[0:40], from_down[0:40]], axis=1)
    from_west = moved(jnp.concatenate([right, corners], axis=0), COL, True)
    from_east = moved(jnp.concatenate([left, corners], axis=0), COL, False)
    sums, pool_lap = call(
        gram, [vmem(POOL, LANES), vmem(POOL, ROWS, LANES)], [VMEM, VMEM], [vmem(416, 192)]
    )(w_near, p_near)
    rows = (smoothing[None, :], active[None, :])
    sent, based, lap = call(
        base,
        [vmem(16, POOL, LANES), vmem(BEAMS, ROWS, LANES), vmem(POOL, ROWS, LANES)],
        [SMEM, SMEM] + [VMEM] * 13,
        [vmem(BEAMS, 8, 512), vmem(POOL, 8, ROWS)],
    )(
        smoothing, active, w_near, pool_lap, sums, *rows,
        top, bottom, left, right, from_up, from_down, from_west, from_east,
    )
    near = exchange(sent, NEAR)
    (sent,) = call(again, [vmem(16, POOL, LANES)], [VMEM])(near)
    far = exchange(sent, FAR)
    final, errors = call(
        finish,
        [far_out(BEAMS, ROWS, LANES), vmem(2, 16, BEAMS)],
        [VMEM] * 10,
        [
            vmem(BEAMS, ROWS, LANES),
            pltpu.VMEM((320, 192), BF16),
            pltpu.VMEM((320, 192), BF16),
            DMA((8,)),
        ],
        [HBM, VMEM],
    )(far, desired.T, plan, beam_ref[None, :], step_size[None, :], *rows, based, p_near, lap)
    return final, jnp.swapaxes(errors, 1, 2)


def solution(mesh):
    split = Mesh(mesh.devices.reshape(4, 2, 4, 8), ("row_0", "row_1", "col_0", "col_1"))
    in_specs = (P(None, ROW, COL), P(None, ROW, COL), P(), P(), P(), P(), P(), P())
    out_specs = (P(None, ROW, COL), P())
    return jax.shard_map(body, mesh=split, in_specs=in_specs, out_specs=out_specs, check_vma=False)
```

```python
import math

import jax
import jax.numpy as jnp
from jax import lax
from jax.experimental import pallas as pl
from jax.experimental.pallas import tpu as pltpu
from jax.sharding import Mesh
from jax.sharding import PartitionSpec as P

NR = 2048
NC = 4096
ROW = ("row_0", "row_1")
COL = ("col_0", "col_1")
NEAR = ("row_1", "col_1")
FAR = ("row_0", "col_0")
SCALE = 1.0 / math.sqrt(NR * NC)
BEAMS, POOL, ROWS, LANES = 40, 12, 256, 128
GROUP = 4
LIMIT = 30 << 20
EXACT = lax.Precision.HIGHEST
NN = (((1,), (0,)), ((), ()))
NT = (((1,), (1,)), ((), ()))
TN = (((0,), (0,)), ((), ()))
F32, BF16 = jnp.float32, jnp.bfloat16
VMEM = pl.BlockSpec(memory_space=pltpu.VMEM)
HBM = pl.BlockSpec(memory_space=pltpu.HBM)
SMEM = pl.BlockSpec(memory_space=pltpu.SMEM)


def iota(shape, dim):
    return lax.broadcasted_iota(jnp.int32, shape, dim)


def dot(a, b, dims, precision=None):
    return lax.dot_general(a, b, dims, precision=precision, preferred_element_type=F32)


def halves(x):
    high = x.astype(BF16)
    return high, (x - high.astype(F32)).astype(BF16)


def thirds(x):
    high = x.astype(BF16)
    rest = x - high.astype(F32)
    mid = rest.astype(BF16)
    return high, mid, (rest - mid.astype(F32)).astype(BF16)


def dot_exact(ones, x, dims):
    return sum(dot(ones.astype(BF16), part, dims) for part in thirds(x))


def exact_dot(x, ones, dims):
    return sum(dot(part, ones.astype(BF16), dims) for part in thirds(x))


def rows_around(x):
    zero = jnp.zeros((1, LANES), F32)
    return jnp.concatenate([x[1:], zero], axis=0) + jnp.concatenate([zero, x[:-1]], axis=0)


def band_matrix(center):
    away = jnp.abs(iota((LANES, LANES), 0) - iota((LANES, LANES), 1))
    return jnp.where(away == 0, center, jnp.where(away == 1, 1.0, 0.0))


def by_side(even, first, second):
    return jnp.where(even, second, first), jnp.where(even, first, second)


def line_ends(w_hbm, pool_hbm, first_ref, second_ref, w_buf, pool_buf, sems):
    copies = []
    for k, at in enumerate((0, ROWS - 8)):
        for j, (src, dst) in enumerate(((w_hbm, w_buf), (pool_hbm, pool_buf))):
            copies.append(pltpu.make_async_copy(src.at[:, at : at + 8, :], dst.at[k], sems.at[2 * k + j]))
    for copy in copies:
        copy.start()
    for copy in copies:
        copy.wait()
    even = lax.axis_index(ROW[1]) == 0
    for rows, buf, top, bottom in (
        (slice(0, 40), w_buf, 0, 7), (slice(40, 80), w_buf, 1, 6), (slice(80, 92), pool_buf, 0, 7)
    ):
        first_ref[rows, :], second_ref[rows, :] = by_side(even, buf[0, :, top, :], buf[1, :, bottom, :])
    for ref in (first_ref, second_ref):
        ref[92:96, :] = jnp.zeros((4, LANES), F32)


def column_ends(w_hbm, pool_hbm, first_ref, second_ref, w_buf, pool_buf, lap_ref, ends_ref, sems):
    copies = [pltpu.make_async_copy(pool_hbm, pool_buf, sems.at[5])]
    for k in range(5):
        copies.append(pltpu.make_async_copy(w_hbm.at[8 * k : 8 * k + 8], w_buf.at[8 * k : 8 * k + 8], sems.at[k]))
    for copy in copies[:2]:
        copy.start()
    row, lane = iota((8, LANES), 0), iota((8, LANES), 1)
    pick = jnp.zeros((8, LANES), F32)
    for k, spot in enumerate((0, LANES - 1, 1, LANES - 2)):
        pick = jnp.where((row == k) & (lane == spot), 1.0, pick)
    pick = pick.astype(BF16)
    pick = jnp.concatenate([pick, pick], axis=1)
    along = band_matrix(-4.0).astype(BF16)
    along = jnp.concatenate([along, along], axis=0)

    def image(p, carry):
        x = pool_buf[p]
        both = jnp.concatenate(halves(x), axis=1)
        ends_ref[BEAMS + p] = dot(pick, both, NT)
        lap_ref[p] = rows_around(x) + dot(both, along, NN)
        return carry

    def beam(b, carry):
        ends_ref[b] = dot(pick, jnp.concatenate(halves(w_buf[b]), axis=1), NT)
        return carry

    for k, copy in enumerate(copies):
        copy.wait()
        if k == 0:
            copies[2].start()
            copies[3].start()
            lax.fori_loop(0, POOL, image, 0, unroll=4)
        else:
            if k + 3 < len(copies):
                copies[k + 3].start()
            lax.fori_loop(8 * k - 8, 8 * k, beam, 0, unroll=4)
    even = (lax.axis_index(COL[1]) & 1) == 0
    for rows, images, left, right in (
        (slice(0, 40), slice(0, 40), 0, 1), (slice(40, 80), slice(0, 40), 2, 3), (slice(80, 92), slice(40, 52), 0, 1)
    ):
        first_ref[rows, :], second_ref[rows, :] = by_side(even, ends_ref[images, left, :], ends_ref[images, right, :])
    for ref in (first_ref, second_ref):
        ref[92:96, :] = jnp.zeros((4, ROWS), F32)


def gram(w_ref, pool_ref, lap_ref, sums_ref, acc_ref):
    acc_ref[...] = jnp.zeros_like(acc_ref)

    def pair(ref, count, t):
        parts = []
        for k in range(GROUP):
            at = pl.multiple_of(t * GROUP * 8 + k * 8, 8)
            parts.append(ref[:, pl.ds(at, 8), :].reshape(count * 8, LANES))
        return jnp.concatenate(parts, axis=1)

    def step(t, carry):
        p_high, p_low = halves(pair(pool_ref, POOL, t))
        l_high, l_low = halves(pair(lap_ref, POOL, t))
        w_high, w_low = halves(pair(w_ref, BEAMS, t))
        a_high = jnp.concatenate([w_high, p_high], axis=0)
        a_low = jnp.concatenate([w_low, p_low], axis=0)
        b_high = jnp.concatenate([p_high, l_high], axis=0)
        b_low = jnp.concatenate([p_low, l_low], axis=0)
        left = jnp.concatenate([a_high, a_high, a_low], axis=1)
        right = jnp.concatenate([b_high, b_low, b_high], axis=1)
        acc_ref[...] += dot(left, right, NT)
        return carry

    lax.fori_loop(0, 32 // GROUP, step, 0)
    n, m = acc_ref.shape
    same = (iota((n, m), 0) & 7) == (iota((n, m), 1) & 7)
    kept = jnp.where(same, acc_ref[...], 0.0)
    q, j = iota((32, m), 0), iota((32, m), 1) >> 3
    fold = jnp.where(((j < POOL) & (q == j)) | ((j >= POOL) & (q == j + 16 - POOL)), 1.0, 0.0)
    folded = dot_exact(fold, kept, NT)
    i, lane = iota((n, LANES), 0) >> 3, iota((n, LANES), 1)
    to_p = jnp.where(((i < BEAMS) & (lane == i)) | ((i >= BEAMS) & (lane == i + 80 - BEAMS)), 1.0, 0.0)
    to_l = jnp.where((i < BEAMS) & (lane == i + 40), 1.0, 0.0)
    sums = exact_dot(folded[0:16], to_p, NN) + exact_dot(folded[16:32], to_l, NN)
    sums_ref[...] = sums[0:POOL]


def again(parts_ref, out_ref):
    sums = parts_ref[0]
    for k in range(1, 16):
        sums = sums + parts_ref[k]
    for k in range(16):
        out_ref[k] = sums


def base(
    smooth_ref, active_ref, w_ref, pool_lap_ref, sums_ref, smooth_row_ref, active_row_ref,
    row_a, row_b, row_a_got, row_b_got, col_a, col_b, col_a_got, col_b_got,
    sent_ref, out_ref, lap_ref, fix_ref, turned_ref, slots_ref,
    top_ref, bottom_ref, up_ref, down_ref, left_ref, right_ref, west_ref, east_ref,
):
    even_row = lax.axis_index(ROW[1]) == 0
    even_col = (lax.axis_index(COL[1]) & 1) == 0
    top_ref[...], bottom_ref[...] = by_side(even_row, row_a[...], row_b[...])
    up_ref[...], down_ref[...] = by_side(even_row, row_a_got[...], row_b_got[...])
    left_ref[...], right_ref[...] = by_side(even_col, col_a[...], col_b[...])
    west_ref[...], east_ref[...] = by_side(even_col, col_a_got[...], col_b_got[...])
    for ref in (west_ref, east_ref):
        one, two = ref[96:136, 0:LANES], ref[96:136, LANES:]
        ref[96:136, 0:LANES], ref[96:136, LANES:] = by_side(even_row, one, two)
    halo = jnp.concatenate([ref[80:96, :] for ref in (west_ref, east_ref, up_ref, down_ref)], axis=1)
    edge = jnp.concatenate([ref[0:40, :] for ref in (left_ref, right_ref, top_ref, bottom_ref)], axis=1)
    edge = jnp.concatenate([jnp.zeros((40, 768), F32), edge, jnp.zeros((48, 768), F32)], axis=0)
    sums = sums_ref[...] + dot(halo, edge, NT, EXACT)[0:POOL]
    for k in range(16):
        sent_ref[k] = sums

    def across(row):
        return jnp.broadcast_to(row, (8, BEAMS)).T[:, 0:1]

    smooth_row, active_row = smooth_row_ref[...], active_row_ref[...]
    live0 = jnp.where(active_row > 0, 1.0, 0.0)
    live1 = jnp.where(active_row > 1, 1.0, 0.0)
    a = across(smooth_row * (live0 + live1))
    c = across(smooth_row * smooth_row * live0 * live1)
    r = lax.axis_index(ROW[0]) * 2 + lax.axis_index(ROW[1])
    k = lax.axis_index(COL[0]) * 8 + lax.axis_index(COL[1])
    has_up, has_down = jnp.where(r > 0, 1.0, 0.0), jnp.where(r < 7, 1.0, 0.0)
    has_west, has_east = jnp.where(k > 0, 1.0, 0.0), jnp.where(k < 31, 1.0, 0.0)
    span, shifted, corner = slice(0, 40), slice(40, 80), slice(96, 136)
    wide, thin = iota((BEAMS, ROWS), 1), iota((BEAMS, LANES), 1)

    def mixed(near, far, own, prev, after):
        return a * near + c * (2.0 * (prev + after) - 8.0 * near + far + own), c * near

    def column(msg_ref, own_ref, far_ref, has):
        near = msg_ref[span, :] - far_ref[span, :]
        prev = jnp.where(wide == 0, 0.0, pltpu.roll(near, 1, 1))
        after = jnp.where(wide == ROWS - 1, 0.0, pltpu.roll(near, ROWS - 1, 1))
        far = msg_ref[shifted, :] - far_ref[shifted, :]
        return mixed(near, far, (has - 1.0) * own_ref[span, :], prev, after)

    def line(msg_ref, own_ref, far_ref, has, at):
        near = msg_ref[span, :] - far_ref[span, :]
        west = pltpu.roll(west_ref[corner, at : at + LANES] - far_ref[span, :], 1, 1)
        east = pltpu.roll(east_ref[corner, at : at + LANES] - far_ref[span, :], LANES - 1, 1)
        prev = jnp.where(thin == 0, west, pltpu.roll(near, 1, 1))
        after = jnp.where(thin == LANES - 1, east, pltpu.roll(near, LANES - 1, 1))
        far = msg_ref[shifted, :] - far_ref[shifted, :]
        return mixed(near, far, (has - 1.0) * own_ref[span, :], prev, after)

    fix_ref[...] = jnp.zeros_like(fix_ref)
    turned_ref[...] = jnp.zeros_like(turned_ref)

    def beams_at(k):
        return pl.ds(k, BEAMS, stride=4)

    def pools_at(k):
        return pl.ds(4 * BEAMS + k, POOL, stride=4)

    east, west = column(east_ref, right_ref, left_ref, has_east), column(west_ref, left_ref, right_ref, has_west)
    for k, (line_of, pool_of) in enumerate(
        ((east[1], None), (east[0], east_ref[80:92, :]), (west[0], west_ref[80:92, :]), (west[1], None))
    ):
        for h in range(2):
            part = slice(LANES * h, LANES * (h + 1))
            turned_ref[h, beams_at(k), :] = line_of[:, part]
            if pool_of is not None:
                turned_ref[h, pools_at(k), :] = pool_of[:, part]
    for k in range(2):
        for h in range(2):
            part = slice(LANES * h, LANES * (h + 1))
            slots_ref[k, part, :] = turned_ref[h, LANES * k : LANES * (k + 1), :].T
    fix_ref[:, 0, 0:128], fix_ref[:, 1, 0:128] = line(up_ref, top_ref, bottom_ref, has_up, 0)
    fix_ref[:, 7, 128:256], fix_ref[:, 6, 128:256] = line(down_ref, bottom_ref, top_ref, has_down, LANES)
    lane = iota((ROWS, LANES), 1)
    at_edge = (lane < 2) | (lane >= LANES - 2)

    def placed(image):
        spun = pltpu.roll(slots_ref[image >> 5], (LANES - 2 - 4 * image) & (LANES - 1), 1)
        return jnp.where(at_edge, spun, 0.0)

    def pool_step(p, carry):
        lap_ref[p] = pool_lap_ref[p] + placed(BEAMS + p)
        return carry

    lax.fori_loop(0, POOL, pool_step, 0, unroll=4)
    lap_ref[:, 0, :] += up_ref[80:92, :]
    lap_ref[:, ROWS - 1, :] += down_ref[80:92, :]

    away = (iota((LANES, LANES), 0) - iota((LANES, LANES), 1)) & (LANES - 1)
    once = jnp.where(away == 0, -2.0, jnp.where((away == 1) | (away == LANES - 1), 1.0, 0.0))
    along = jnp.concatenate([once, dot(once, once, NN)], axis=1).astype(BF16)
    along = jnp.concatenate([along, along], axis=0)

    def around(x):
        return pltpu.roll(x, 1, 0) + pltpu.roll(x, ROWS - 1, 0)

    def beam(b, carry):
        s_b, n_b = smooth_ref[b], active_ref[b]
        r_0, r_1 = jnp.where(n_b > 0, s_b, 0.0), jnp.where(n_b > 1, s_b, 0.0)
        a_b, c_b = r_0 + r_1, r_0 * r_1
        x = w_ref[b]
        sides = dot(jnp.concatenate(halves(x), axis=1), along, NN)
        one, two = sides[:, :LANES], sides[:, LANES:]
        lines = around(x)
        inner = around((a_b - 2.0 * c_b) * x + (2.0 * c_b) * one + c_b * lines)
        kept = (1.0 - 2.0 * a_b + 4.0 * c_b) * x + (a_b - 4.0 * c_b) * one + c_b * two - (2.0 * c_b) * lines
        out = kept + inner + placed(b)
        out_ref[b, 8 : ROWS - 8, :] = out[8 : ROWS - 8]
        out_ref[b, 0:8, :] = out[0:8] + fix_ref[b, :, 0:128]
        out_ref[b, ROWS - 8 : ROWS, :] = out[ROWS - 8 :] + fix_ref[b, :, 128:256]
        return carry

    lax.fori_loop(0, BEAMS, beam, 0, unroll=2)


def finish(
    parts_ref, desired_ref, plan_ref, ref_ref, rate_ref, smooth_ref, active_ref, base_ref, pool_ref, lap_ref,
    out_hbm, err_ref, done_ref, high_ref, low_ref, sems,
):
    def store(t):
        at = pl.ds(pl.multiple_of(t * 32, 8), 32)
        return pltpu.make_async_copy(done_ref.at[:, at, :], out_hbm.at[:, at, :], sems.at[t])

    sums = parts_ref[0]
    for k in range(1, 16):
        sums = sums + parts_ref[k]
    one_hot = jnp.where(iota((8, BEAMS), 0) == ref_ref[...], 1.0, 0.0)
    target = dot(desired_ref[...], one_hot, TN, EXACT)
    rate, smooth = rate_ref[...] * SCALE, smooth_ref[...]
    live0 = jnp.where(active_ref[...] > 0, 1.0, 0.0)
    live1 = jnp.where(active_ref[...] > 1, 1.0, 0.0)
    hits = [jnp.where(iota((POOL, 16), 0) == plan_ref[t : t + 1, :], 1.0, 0.0) for t in range(2)]
    many = [jnp.sum(h, axis=1, keepdims=True) for h in hits]
    p0 = sums[:, 0:BEAMS]
    lap = pltpu.roll(sums, LANES - 40, 1)[:, 0:BEAMS]
    inner = pltpu.roll(sums, LANES - 80, 1)[:, 0:POOL]
    e0 = target - SCALE * p0
    c0 = many[0] * e0
    p1 = p0 + live0 * (rate * dot(inner, c0, NN, EXACT) + smooth * lap)
    e1 = target - SCALE * p1
    c1 = many[1] * e1
    for t, e in enumerate((e0, e1)):
        err_ref[t] = dot(hits[t], e, TN, EXACT)
    d0 = rate * (live0 * c0 + live1 * c1)
    d1 = live0 * live1 * rate * smooth * c0
    gap = jnp.zeros((4, BEAMS), F32)
    both = jnp.concatenate([d0, gap, d1, gap], axis=0)
    spread = jnp.where((iota((320, BEAMS), 0) >> 3) == iota((320, BEAMS), 1), 1.0, 0.0)
    spread = spread.astype(BF16)
    q, j = iota((32, 192), 0), iota((32, 192), 1) >> 3
    fold = jnp.where(((j < POOL) & (q == j)) | ((j >= POOL) & (q == j + 16 - POOL)), 1.0, 0.0).astype(BF16)
    same = (iota((320, 192), 0) & 7) == (iota((320, 192), 1) & 7)
    for ref, part in zip((high_ref, low_ref), halves(both)):
        by_q = dot(spread, part, NT).astype(BF16)
        ref[...] = jnp.where(same, dot(by_q, fold, NN), 0.0).astype(BF16)

    def step(t, carry):
        def tile(ref, at):
            return ref.at[:, pl.ds(pl.multiple_of(t * 32 + at, 8), 8), :]

        for k in range(2):
            halves_of = []
            for h in range(2):
                at = 16 * k + 8 * h
                halves_of.append(
                    jnp.concatenate([tile(ref, at)[...].reshape(96, LANES) for ref in (pool_ref, lap_ref)], axis=0)
                )
            high, low = halves(jnp.concatenate(halves_of, axis=1))
            got = dot(high_ref[...], high, NN) + dot(high_ref[...], low, NN) + dot(low_ref[...], high, NN)
            for h in range(2):
                part = got[:, h * LANES : (h + 1) * LANES].reshape(BEAMS, 8, LANES)
                at = 16 * k + 8 * h
                tile(done_ref, at)[...] = tile(base_ref, at)[...] + part
        store(t).start()
        return carry

    lax.fori_loop(0, 8, step, 0)
    for t in range(8):
        store(t).wait()


def call(kernel, outs, specs, scratch=(), out_specs=None):
    run = pl.pallas_call(
        kernel,
        name=kernel.__name__,
        out_shape=outs,
        in_specs=specs,
        out_specs=out_specs or [VMEM] * len(outs),
        scratch_shapes=scratch,
        compiler_params=pltpu.CompilerParams(vmem_limit_bytes=LIMIT),
    )
    homes = {id(VMEM): pltpu.VMEM, id(HBM): pltpu.HBM}

    def at_home(value, spec):
        return pltpu.with_memory_space_constraint(value, homes[id(spec)]) if id(spec) in homes else value

    return lambda *args: run(*[at_home(x, spec) for x, spec in zip(args, specs)])


def vmem(*dims):
    return pltpu.VMEM(dims, F32)


def far_out(*dims):
    return pltpu.HBM(dims, F32)


def swapped(value, axes, phase):
    count = lax.axis_size(axes)
    pairs = [(i, i + 1) for i in range(phase, count - 1, 2)]
    return lax.ppermute(value, axes, pairs + [(b, a) for a, b in pairs])


def exchange(value, axes):
    return lax.all_to_all(value, axes, split_axis=0, concat_axis=0, tiled=True)


def body(weights, pool, desired, plan, beam_ref, step_size, smoothing, active):
    DMA = pltpu.SemaphoreType.DMA
    row_a, row_b = call(
        line_ends,
        [vmem(96, LANES)] * 2,
        [HBM, HBM],
        [vmem(2, BEAMS, 8, LANES), vmem(2, POOL, 8, LANES), DMA((4,))],
    )(weights, pool)
    row_b_got = swapped(row_b, ROW, 1)
    row_a_got = swapped(row_a, ROW, 0)
    col_a, col_b, w_near, p_near, pool_lap = call(
        column_ends,
        [vmem(96, ROWS)] * 2 + [vmem(BEAMS, ROWS, LANES), vmem(POOL, ROWS, LANES), vmem(POOL, ROWS, LANES)],
        [HBM, HBM],
        [vmem(BEAMS + POOL, 8, ROWS), DMA((6,))],
    )(weights, pool)
    corners = jnp.concatenate([row_a_got[0:40], row_b_got[0:40]], axis=1)
    col_a_got = swapped(jnp.concatenate([col_a, corners], axis=0), COL, 0)
    col_b_got = swapped(jnp.concatenate([col_b, corners], axis=0), COL, 1)
    (sums,) = call(gram, [vmem(POOL, LANES)], [VMEM] * 3, [vmem(416, 192)])(w_near, p_near, pool_lap)
    rows = (smoothing[None, :], active[None, :])
    sent, based, lap = call(
        base,
        [vmem(16, POOL, LANES), vmem(BEAMS, ROWS, LANES), vmem(POOL, ROWS, LANES)],
        [SMEM, SMEM] + [VMEM] * 13,
        [vmem(BEAMS, 8, 256), vmem(2, 256, LANES), vmem(2, ROWS, LANES)]
        + [vmem(96, LANES)] * 4 + [vmem(96, ROWS)] * 2 + [vmem(136, ROWS)] * 2,
    )(
        smoothing, active, w_near, pool_lap, sums, *rows,
        row_a, row_b, row_a_got, row_b_got, col_a, col_b, col_a_got, col_b_got,
    )
    near = exchange(sent, NEAR)
    (sent,) = call(again, [vmem(16, POOL, LANES)], [VMEM])(near)
    far = exchange(sent, FAR)
    final, errors = call(
        finish,
        [far_out(BEAMS, ROWS, LANES), jax.ShapeDtypeStruct((2, 16, BEAMS), F32)],
        [VMEM] * 10,
        [
            vmem(BEAMS, ROWS, LANES),
            pltpu.VMEM((320, 192), BF16),
            pltpu.VMEM((320, 192), BF16),
            DMA((8,)),
        ],
        [HBM, VMEM],
    )(far, desired.T, plan, beam_ref[None, :], step_size[None, :], *rows, based, p_near, lap)
    return final, jnp.swapaxes(errors, 1, 2)


def solution(mesh):
    split = Mesh(mesh.devices.reshape(4, 2, 4, 8), ("row_0", "row_1", "col_0", "col_1"))
    in_specs = (P(None, ROW, COL), P(None, ROW, COL), P(), P(), P(), P(), P(), P())
    out_specs = (P(None, ROW, COL), P())
    return jax.shard_map(body, mesh=split, in_specs=in_specs, out_specs=out_specs, check_vma=False)
```

```python
import functools
import math

import jax
import jax.numpy as jnp
from jax import lax
from jax.experimental import pallas as pl
from jax.experimental.pallas import tpu as pltpu
from jax.sharding import Mesh
from jax.sharding import PartitionSpec as P

NR = 2048
NC = 4096
ROW = ("row_0", "row_1")
COL = ("col_0", "col_1")
NEAR = ("row_1", "col_1")
FAR = ("row_0", "col_0")
SCALE = 1.0 / math.sqrt(NR * NC)
BEAMS, POOL, ROWS, LANES = 40, 12, 256, 128
GROUP = 4
LIMIT = 30 << 20
FIRST, CHUNK = 16, 4
EXACT = lax.Precision.HIGHEST
NN = (((1,), (0,)), ((), ()))
NT = (((1,), (1,)), ((), ()))
TN = (((0,), (0,)), ((), ()))
F32, BF16 = jnp.float32, jnp.bfloat16
VMEM = pl.BlockSpec(memory_space=pltpu.VMEM)
HBM = pl.BlockSpec(memory_space=pltpu.HBM)
SMEM = pl.BlockSpec(memory_space=pltpu.SMEM)


def iota(shape, dim):
    return lax.broadcasted_iota(jnp.int32, shape, dim)


def dot(a, b, dims, precision=None):
    return lax.dot_general(a, b, dims, precision=precision, preferred_element_type=F32)


def halves(x):
    high = x.astype(BF16)
    return high, (x - high.astype(F32)).astype(BF16)


def thirds(x):
    high = x.astype(BF16)
    rest = x - high.astype(F32)
    mid = rest.astype(BF16)
    return high, mid, (rest - mid.astype(F32)).astype(BF16)


def dot_exact(ones, x, dims):
    return sum(dot(ones.astype(BF16), part, dims) for part in thirds(x))


def exact_dot(x, ones, dims):
    return sum(dot(part, ones.astype(BF16), dims) for part in thirds(x))


def rows_around(x):
    zero = jnp.zeros((1, LANES), F32)
    return jnp.concatenate([x[1:], zero], axis=0) + jnp.concatenate([zero, x[:-1]], axis=0)


def band_matrix(center):
    away = jnp.abs(iota((LANES, LANES), 0) - iota((LANES, LANES), 1))
    return jnp.where(away == 0, center, jnp.where(away == 1, 1.0, 0.0))


def by_side(even, first, second):
    return jnp.where(even, second, first), jnp.where(even, first, second)


def line_ends(w_hbm, pool_hbm, first_ref, second_ref, w_buf, pool_buf, sems):
    copies = []
    for k, at in enumerate((0, ROWS - 8)):
        for j, (src, dst) in enumerate(((w_hbm, w_buf), (pool_hbm, pool_buf))):
            copies.append(pltpu.make_async_copy(src.at[:, at : at + 8, :], dst.at[k], sems.at[2 * k + j]))
    for copy in copies:
        copy.start()
    for copy in copies:
        copy.wait()
    even = lax.axis_index(ROW[1]) == 0
    for rows, buf, top, bottom in (
        (slice(0, 40), w_buf, 0, 7), (slice(40, 80), w_buf, 1, 6), (slice(80, 92), pool_buf, 0, 7)
    ):
        first_ref[rows, :], second_ref[rows, :] = by_side(even, buf[0, :, top, :], buf[1, :, bottom, :])
    for ref in (first_ref, second_ref):
        ref[92:96, :] = jnp.zeros((4, LANES), F32)


def column_ends(w_hbm, pool_hbm, first_ref, second_ref, w_buf, pool_buf, lap_ref, ends_ref, sems):
    copies = [pltpu.make_async_copy(pool_hbm, pool_buf, sems.at[5])]
    for k in range(5):
        copies.append(pltpu.make_async_copy(w_hbm.at[8 * k : 8 * k + 8], w_buf.at[8 * k : 8 * k + 8], sems.at[k]))
    for copy in copies[:2]:
        copy.start()
    row, lane = iota((8, LANES), 0), iota((8, LANES), 1)
    pick = jnp.zeros((8, LANES), F32)
    for k, spot in enumerate((0, LANES - 1, 1, LANES - 2)):
        pick = jnp.where((row == k) & (lane == spot), 1.0, pick)
    pick = pick.astype(BF16)
    pick = jnp.concatenate([pick, pick], axis=1)
    along = band_matrix(-4.0).astype(BF16)
    along = jnp.concatenate([along, along], axis=0)

    def image(p, carry):
        x = pool_buf[p]
        both = jnp.concatenate(halves(x), axis=1)
        ends_ref[BEAMS + p] = dot(pick, both, NT)
        lap_ref[p] = rows_around(x) + dot(both, along, NN)
        return carry

    def beam(b, carry):
        ends_ref[b] = dot(pick, jnp.concatenate(halves(w_buf[b]), axis=1), NT)
        return carry

    for k, copy in enumerate(copies):
        copy.wait()
        if k == 0:
            copies[2].start()
            copies[3].start()
            lax.fori_loop(0, POOL, image, 0, unroll=4)
        else:
            if k + 3 < len(copies):
                copies[k + 3].start()
            lax.fori_loop(8 * k - 8, 8 * k, beam, 0, unroll=4)
    even = (lax.axis_index(COL[1]) & 1) == 0
    for rows, images, left, right in (
        (slice(0, 40), slice(0, 40), 0, 1), (slice(40, 80), slice(0, 40), 2, 3), (slice(80, 92), slice(40, 52), 0, 1)
    ):
        first_ref[rows, :], second_ref[rows, :] = by_side(even, ends_ref[images, left, :], ends_ref[images, right, :])
    for ref in (first_ref, second_ref):
        ref[92:96, :] = jnp.zeros((4, ROWS), F32)


def gram(w_ref, pool_ref, lap_ref, sums_ref, lap_hbm, acc_ref, sem):
    keep = pltpu.make_async_copy(lap_ref, lap_hbm, sem)
    keep.start()
    acc_ref[...] = jnp.zeros_like(acc_ref)

    def pair(ref, count, t):
        parts = []
        for k in range(GROUP):
            at = pl.multiple_of(t * GROUP * 8 + k * 8, 8)
            parts.append(ref[:, pl.ds(at, 8), :].reshape(count * 8, LANES))
        return jnp.concatenate(parts, axis=1)

    def step(t, carry):
        p_high, p_low = halves(pair(pool_ref, POOL, t))
        l_high, l_low = halves(pair(lap_ref, POOL, t))
        w_high, w_low = halves(pair(w_ref, BEAMS, t))
        a_high = jnp.concatenate([w_high, p_high], axis=0)
        a_low = jnp.concatenate([w_low, p_low], axis=0)
        b_high = jnp.concatenate([p_high, l_high], axis=0)
        b_low = jnp.concatenate([p_low, l_low], axis=0)
        left = jnp.concatenate([a_high, a_high, a_low], axis=1)
        right = jnp.concatenate([b_high, b_low, b_high], axis=1)
        acc_ref[...] += dot(left, right, NT)
        return carry

    lax.fori_loop(0, 32 // GROUP, step, 0)
    n, m = acc_ref.shape
    same = (iota((n, m), 0) & 7) == (iota((n, m), 1) & 7)
    kept = jnp.where(same, acc_ref[...], 0.0)
    q, j = iota((32, m), 0), iota((32, m), 1) >> 3
    fold = jnp.where(((j < POOL) & (q == j)) | ((j >= POOL) & (q == j + 16 - POOL)), 1.0, 0.0)
    folded = dot_exact(fold, kept, NT)
    i, lane = iota((n, LANES), 0) >> 3, iota((n, LANES), 1)
    to_p = jnp.where(((i < BEAMS) & (lane == i)) | ((i >= BEAMS) & (lane == i + 80 - BEAMS)), 1.0, 0.0)
    to_l = jnp.where((i < BEAMS) & (lane == i + 40), 1.0, 0.0)
    sums = exact_dot(folded[0:16], to_p, NN) + exact_dot(folded[16:32], to_l, NN)
    sums_ref[...] = sums[0:POOL]
    keep.wait()


def cross(
    sums_ref, row_a, row_b, row_a_got, row_b_got, col_a, col_b, col_a_got, col_b_got, sent_ref
):
    even_row = lax.axis_index(ROW[1]) == 0
    even_col = (lax.axis_index(COL[1]) & 1) == 0
    halo, edge = [], []
    for even, got, own in ((even_col, (col_a_got, col_b_got), (col_a, col_b)), (even_row, (row_a_got, row_b_got), (row_a, row_b))):
        halo.extend(by_side(even, *[ref[80:96, :] for ref in got]))
        edge.extend(by_side(even, *[ref[0:40, :] for ref in own]))
    edge = jnp.concatenate(edge, axis=1)
    edge = jnp.concatenate([jnp.zeros((40, 768), F32), edge, jnp.zeros((48, 768), F32)], axis=0)
    sums = sums_ref[...] + dot(jnp.concatenate(halo, axis=1), edge, NT, EXACT)[0:POOL]
    for k in range(16):
        sent_ref[k] = sums


def again(parts_ref, token_ref, out_ref):
    sums = parts_ref[0]
    for k in range(1, 16):
        sums = sums + parts_ref[k]
    for k in range(16):
        out_ref[k] = sums


def base(first, count, with_pool, smooth_ref, active_ref, w_hbm, lap_in_hbm, smooth_row_ref, active_row_ref, row_a, row_b, row_a_got, row_b_got, col_a, col_b, col_a_got, col_b_got, *rest):
    if with_pool:
        out_hbm, lap_hbm, token_ref, *rest, lap_ref = rest
    else:
        out_hbm, *rest = rest
    (
        fix_ref, turned_ref, slots_ref, top_ref, bottom_ref, up_ref, down_ref, left_ref, right_ref, west_ref, east_ref,
        w_ref, out_ref, sems,
    ) = rest
    parts = count // CHUNK
    loads, stores = [], []
    for k in range(parts):
        part = slice(CHUNK * k, CHUNK * (k + 1))
        source = w_hbm.at[first + CHUNK * k : first + CHUNK * (k + 1)]
        loads.append(pltpu.make_async_copy(source, w_ref.at[part], sems.at[0, k]))
        stores.append(pltpu.make_async_copy(out_ref.at[part], out_hbm.at[part], sems.at[1, k]))
    for copy in loads[:3]:
        copy.start()
    if with_pool:
        load_lap = pltpu.make_async_copy(lap_in_hbm, lap_ref, sems.at[0, parts])
        store_lap = pltpu.make_async_copy(lap_ref, lap_hbm, sems.at[1, parts])
        load_lap.start()
    even_row = lax.axis_index(ROW[1]) == 0
    even_col = (lax.axis_index(COL[1]) & 1) == 0
    top_ref[...], bottom_ref[...] = by_side(even_row, row_a[...], row_b[...])
    up_ref[...], down_ref[...] = by_side(even_row, row_a_got[...], row_b_got[...])
    left_ref[...], right_ref[...] = by_side(even_col, col_a[...], col_b[...])
    west_ref[...], east_ref[...] = by_side(even_col, col_a_got[...], col_b_got[...])
    for ref in (west_ref, east_ref):
        one, two = ref[96:136, 0:LANES], ref[96:136, LANES:]
        ref[96:136, 0:LANES], ref[96:136, LANES:] = by_side(even_row, one, two)
    def across(row):
        return jnp.broadcast_to(row, (8, BEAMS)).T[:, 0:1]

    smooth_row, active_row = smooth_row_ref[...], active_row_ref[...]
    live0 = jnp.where(active_row > 0, 1.0, 0.0)
    live1 = jnp.where(active_row > 1, 1.0, 0.0)
    a = across(smooth_row * (live0 + live1))
    c = across(smooth_row * smooth_row * live0 * live1)
    r = lax.axis_index(ROW[0]) * 2 + lax.axis_index(ROW[1])
    k = lax.axis_index(COL[0]) * 8 + lax.axis_index(COL[1])
    has_up, has_down = jnp.where(r > 0, 1.0, 0.0), jnp.where(r < 7, 1.0, 0.0)
    has_west, has_east = jnp.where(k > 0, 1.0, 0.0), jnp.where(k < 31, 1.0, 0.0)
    span, shifted, corner = slice(0, 40), slice(40, 80), slice(96, 136)
    wide, thin = iota((BEAMS, ROWS), 1), iota((BEAMS, LANES), 1)

    def mixed(near, far, own, prev, after):
        return a * near + c * (2.0 * (prev + after) - 8.0 * near + far + own), c * near

    def column(msg_ref, own_ref, far_ref, has):
        near = msg_ref[span, :] - far_ref[span, :]
        prev = jnp.where(wide == 0, 0.0, pltpu.roll(near, 1, 1))
        after = jnp.where(wide == ROWS - 1, 0.0, pltpu.roll(near, ROWS - 1, 1))
        far = msg_ref[shifted, :] - far_ref[shifted, :]
        return mixed(near, far, (has - 1.0) * own_ref[span, :], prev, after)

    def line(msg_ref, own_ref, far_ref, has, at):
        near = msg_ref[span, :] - far_ref[span, :]
        west = pltpu.roll(west_ref[corner, at : at + LANES] - far_ref[span, :], 1, 1)
        east = pltpu.roll(east_ref[corner, at : at + LANES] - far_ref[span, :], LANES - 1, 1)
        prev = jnp.where(thin == 0, west, pltpu.roll(near, 1, 1))
        after = jnp.where(thin == LANES - 1, east, pltpu.roll(near, LANES - 1, 1))
        far = msg_ref[shifted, :] - far_ref[shifted, :]
        return mixed(near, far, (has - 1.0) * own_ref[span, :], prev, after)

    fix_ref[...] = jnp.zeros_like(fix_ref)
    turned_ref[...] = jnp.zeros_like(turned_ref)

    def beams_at(k):
        return pl.ds(k, BEAMS, stride=4)

    def pools_at(k):
        return pl.ds(4 * BEAMS + k, POOL, stride=4)

    east, west = column(east_ref, right_ref, left_ref, has_east), column(west_ref, left_ref, right_ref, has_west)
    for k, (line_of, pool_of) in enumerate(
        ((east[1], None), (east[0], east_ref[80:92, :]), (west[0], west_ref[80:92, :]), (west[1], None))
    ):
        for h in range(2):
            part = slice(LANES * h, LANES * (h + 1))
            turned_ref[h, beams_at(k), :] = line_of[:, part]
            if pool_of is not None:
                turned_ref[h, pools_at(k), :] = pool_of[:, part]
    for k in range(2):
        for h in range(2):
            part = slice(LANES * h, LANES * (h + 1))
            slots_ref[k, part, :] = turned_ref[h, LANES * k : LANES * (k + 1), :].T
    fix_ref[:, 0, 0:128], fix_ref[:, 1, 0:128] = line(up_ref, top_ref, bottom_ref, has_up, 0)
    fix_ref[:, 7, 128:256], fix_ref[:, 6, 128:256] = line(down_ref, bottom_ref, top_ref, has_down, LANES)
    lane = iota((ROWS, LANES), 1)
    at_edge = (lane < 2) | (lane >= LANES - 2)

    def placed(image):
        spun = pltpu.roll(slots_ref[image >> 5], (LANES - 2 - 4 * image) & (LANES - 1), 1)
        return jnp.where(at_edge, spun, 0.0)

    away = (iota((LANES, LANES), 0) - iota((LANES, LANES), 1)) & (LANES - 1)
    once = jnp.where(away == 0, -2.0, jnp.where((away == 1) | (away == LANES - 1), 1.0, 0.0))
    along = jnp.concatenate([once, dot(once, once, NN)], axis=1).astype(BF16)
    along = jnp.concatenate([along, along], axis=0)

    def around(x):
        return pltpu.roll(x, 1, 0) + pltpu.roll(x, ROWS - 1, 0)

    def beam(b, carry):
        s_b, n_b = smooth_ref[first + b], active_ref[first + b]
        r_0, r_1 = jnp.where(n_b > 0, s_b, 0.0), jnp.where(n_b > 1, s_b, 0.0)
        a_b, c_b = r_0 + r_1, r_0 * r_1
        x = w_ref[b]
        sides = dot(jnp.concatenate(halves(x), axis=1), along, NN)
        one, two = sides[:, :LANES], sides[:, LANES:]
        lines = around(x)
        inner = around((a_b - 2.0 * c_b) * x + (2.0 * c_b) * one + c_b * lines)
        kept = (1.0 - 2.0 * a_b + 4.0 * c_b) * x + (a_b - 4.0 * c_b) * one + c_b * two - (2.0 * c_b) * lines
        out = kept + inner + placed(first + b)
        out_ref[b, 8 : ROWS - 8, :] = out[8 : ROWS - 8]
        out_ref[b, 0:8, :] = out[0:8] + fix_ref[first + b, :, 0:128]
        out_ref[b, ROWS - 8 : ROWS, :] = out[ROWS - 8 :] + fix_ref[first + b, :, 128:256]
        return carry

    for k in range(parts):
        loads[k].wait()
        if k + 3 < parts:
            loads[k + 3].start()
        lax.fori_loop(CHUNK * k, CHUNK * (k + 1), beam, 0, unroll=2)
        stores[k].start()
        if k == 0 and with_pool:
            load_lap.wait()

            def pool_step(p, carry):
                lap_ref[p] = lap_ref[p] + placed(BEAMS + p)
                return carry

            lax.fori_loop(0, POOL, pool_step, 0, unroll=4)
            lap_ref[:, 0, :] += up_ref[80:92, :]
            lap_ref[:, ROWS - 1, :] += down_ref[80:92, :]
            store_lap.start()
    for store in stores:
        store.wait()
    if with_pool:
        store_lap.wait()
        token_ref[...] = jnp.zeros_like(token_ref)


def finish(
    parts_ref, desired_ref, plan_ref, ref_ref, rate_ref, smooth_ref, active_ref, base_a_hbm, base_b_hbm, pool_hbm,
    lap_hbm, out_hbm, err_ref, base_ref, pool_ref, lap_ref, high_ref, low_ref, in_sems, out_sems,
):
    def rows_of(t):
        return pl.ds(pl.multiple_of(t * 32, 8), 32)

    def fetches(t):
        cut = base_a_hbm.shape[0]
        at = rows_of(t)
        pairs = (
            (base_a_hbm.at[:, at, :], base_ref.at[0:cut, at, :]),
            (base_b_hbm.at[:, at, :], base_ref.at[cut:BEAMS, at, :]),
            (pool_hbm.at[:, at, :], pool_ref.at[:, at, :]),
            (lap_hbm.at[:, at, :], lap_ref.at[:, at, :]),
        )
        return [pltpu.make_async_copy(src, dst, in_sems.at[k, t]) for k, (src, dst) in enumerate(pairs)]

    def store(t):
        at = rows_of(t)
        return pltpu.make_async_copy(base_ref.at[:, at, :], out_hbm.at[:, at, :], out_sems.at[t])

    for t in range(8):
        for copy in fetches(t):
            copy.start()

    sums = parts_ref[0]
    for k in range(1, 16):
        sums = sums + parts_ref[k]
    one_hot = jnp.where(iota((8, BEAMS), 0) == ref_ref[...], 1.0, 0.0)
    target = dot(desired_ref[...], one_hot, TN, EXACT)
    rate, smooth = rate_ref[...] * SCALE, smooth_ref[...]
    live0 = jnp.where(active_ref[...] > 0, 1.0, 0.0)
    live1 = jnp.where(active_ref[...] > 1, 1.0, 0.0)
    hits = [jnp.where(iota((POOL, 16), 0) == plan_ref[t : t + 1, :], 1.0, 0.0) for t in range(2)]
    many = [jnp.sum(h, axis=1, keepdims=True) for h in hits]
    p0 = sums[:, 0:BEAMS]
    lap = pltpu.roll(sums, LANES - 40, 1)[:, 0:BEAMS]
    inner = pltpu.roll(sums, LANES - 80, 1)[:, 0:POOL]
    e0 = target - SCALE * p0
    c0 = many[0] * e0
    p1 = p0 + live0 * (rate * dot(inner, c0, NN, EXACT) + smooth * lap)
    e1 = target - SCALE * p1
    c1 = many[1] * e1
    for t, e in enumerate((e0, e1)):
        err_ref[t] = dot(hits[t], e, TN, EXACT)
    d0 = rate * (live0 * c0 + live1 * c1)
    d1 = live0 * live1 * rate * smooth * c0
    gap = jnp.zeros((4, BEAMS), F32)
    both = jnp.concatenate([d0, gap, d1, gap], axis=0)
    spread = jnp.where((iota((320, BEAMS), 0) >> 3) == iota((320, BEAMS), 1), 1.0, 0.0)
    spread = spread.astype(BF16)
    q, j = iota((32, 192), 0), iota((32, 192), 1) >> 3
    fold = jnp.where(((j < POOL) & (q == j)) | ((j >= POOL) & (q == j + 16 - POOL)), 1.0, 0.0).astype(BF16)
    same = (iota((320, 192), 0) & 7) == (iota((320, 192), 1) & 7)
    for ref, part in zip((high_ref, low_ref), halves(both)):
        by_q = dot(spread, part, NT).astype(BF16)
        ref[...] = jnp.where(same, dot(by_q, fold, NN), 0.0).astype(BF16)

    def step(t, carry):
        for copy in fetches(t):
            copy.wait()

        def tile(ref, at):
            return ref.at[:, pl.ds(pl.multiple_of(t * 32 + at, 8), 8), :]

        for k in range(2):
            halves_of = []
            for h in range(2):
                at = 16 * k + 8 * h
                halves_of.append(
                    jnp.concatenate([tile(ref, at)[...].reshape(96, LANES) for ref in (pool_ref, lap_ref)], axis=0)
                )
            high, low = halves(jnp.concatenate(halves_of, axis=1))
            got = dot(high_ref[...], high, NN) + dot(high_ref[...], low, NN) + dot(low_ref[...], high, NN)
            for h in range(2):
                part = got[:, h * LANES : (h + 1) * LANES].reshape(BEAMS, 8, LANES)
                tile(base_ref, 16 * k + 8 * h)[...] += part
        store(t).start()
        return carry

    lax.fori_loop(0, 8, step, 0)
    for t in range(8):
        store(t).wait()


def call(kernel, outs, specs, scratch=(), out_specs=None):
    run = pl.pallas_call(
        kernel,
        name=getattr(kernel, "__name__", "base"),
        out_shape=outs,
        in_specs=specs,
        out_specs=out_specs or [VMEM] * len(outs),
        scratch_shapes=scratch,
        compiler_params=pltpu.CompilerParams(vmem_limit_bytes=LIMIT),
    )
    homes = {id(VMEM): pltpu.VMEM, id(HBM): pltpu.HBM}

    def at_home(value, spec):
        return pltpu.with_memory_space_constraint(value, homes[id(spec)]) if id(spec) in homes else value

    return lambda *args: run(*[at_home(x, spec) for x, spec in zip(args, specs)])


def vmem(*dims):
    return pltpu.VMEM(dims, F32)


def far_out(*dims):
    return pltpu.HBM(dims, F32)


def swapped(value, axes, phase):
    count = lax.axis_size(axes)
    pairs = [(i, i + 1) for i in range(phase, count - 1, 2)]
    return lax.ppermute(value, axes, pairs + [(b, a) for a, b in pairs])


def exchange(value, axes):
    return lax.all_to_all(value, axes, split_axis=0, concat_axis=0, tiled=True)


def body(weights, pool, desired, plan, beam_ref, step_size, smoothing, active):
    DMA = pltpu.SemaphoreType.DMA
    row_a, row_b = call(
        line_ends,
        [vmem(96, LANES)] * 2,
        [HBM, HBM],
        [vmem(2, BEAMS, 8, LANES), vmem(2, POOL, 8, LANES), DMA((4,))],
    )(weights, pool)
    row_b_got = swapped(row_b, ROW, 1)
    row_a_got = swapped(row_a, ROW, 0)
    col_a, col_b, w_near, p_near, pool_lap = call(
        column_ends,
        [vmem(96, ROWS)] * 2 + [vmem(BEAMS, ROWS, LANES), vmem(POOL, ROWS, LANES), vmem(POOL, ROWS, LANES)],
        [HBM, HBM],
        [vmem(BEAMS + POOL, 8, ROWS), DMA((6,))],
    )(weights, pool)
    corners = jnp.concatenate([row_a_got[0:40], row_b_got[0:40]], axis=1)
    col_a_got = swapped(jnp.concatenate([col_a, corners], axis=0), COL, 0)
    col_b_got = swapped(jnp.concatenate([col_b, corners], axis=0), COL, 1)
    sums, pool_lap = call(
        gram,
        [vmem(POOL, LANES), far_out(POOL, ROWS, LANES)],
        [VMEM] * 3,
        [vmem(416, 192), DMA],
        [VMEM, HBM],
    )(w_near, p_near, pool_lap)
    edges = (row_a, row_b, row_a_got, row_b_got, col_a, col_b, col_a_got, col_b_got)
    (sent,) = call(cross, [vmem(16, POOL, LANES)], [VMEM] * 9)(sums, *edges)
    near = exchange(sent, NEAR)
    rows = (smoothing[None, :], active[None, :])
    shared = (smoothing, active, weights, pool_lap, *rows, *edges)
    specs = [SMEM, SMEM, HBM, HBM] + [VMEM] * 10
    edge_scratch = (
        [vmem(BEAMS, 8, 256), vmem(2, 256, LANES), vmem(2, ROWS, LANES)]
        + [vmem(96, LANES)] * 4 + [vmem(96, ROWS)] * 2 + [vmem(136, ROWS)] * 2
    )
    rest = BEAMS - FIRST
    based_a, lap, token = call(
        functools.partial(base, 0, FIRST, True),
        [far_out(FIRST, ROWS, LANES), far_out(POOL, ROWS, LANES), vmem(8, LANES)],
        specs,
        edge_scratch + [vmem(FIRST, ROWS, LANES)] * 2 + [DMA((2, FIRST // CHUNK + 1)), vmem(POOL, ROWS, LANES)],
        [HBM, HBM, VMEM],
    )(*shared)
    (sent,) = call(again, [vmem(16, POOL, LANES)], [VMEM] * 2)(near, token)
    far = exchange(sent, FAR)
    (based_b,) = call(
        functools.partial(base, FIRST, rest, False),
        [far_out(rest, ROWS, LANES)],
        specs,
        edge_scratch + [vmem(rest, ROWS, LANES)] * 2 + [DMA((2, rest // CHUNK))],
        [HBM],
    )(*shared)
    final, errors = call(
        finish,
        [far_out(BEAMS, ROWS, LANES), jax.ShapeDtypeStruct((2, 16, BEAMS), F32)],
        [VMEM] * 7 + [HBM] * 4,
        [
            vmem(BEAMS, ROWS, LANES),
            vmem(POOL, ROWS, LANES),
            vmem(POOL, ROWS, LANES),
            pltpu.VMEM((320, 192), BF16),
            pltpu.VMEM((320, 192), BF16),
            DMA((4, 8)),
            DMA((8,)),
        ],
        [HBM, VMEM],
    )(far, desired.T, plan, beam_ref[None, :], step_size[None, :], *rows, based_a, based_b, pool, lap)
    return final, jnp.swapaxes(errors, 1, 2)


def solution(mesh):
    split = Mesh(mesh.devices.reshape(4, 2, 4, 8), ("row_0", "row_1", "col_0", "col_1"))
    in_specs = (P(None, ROW, COL), P(None, ROW, COL), P(), P(), P(), P(), P(), P())
    out_specs = (P(None, ROW, COL), P())
    return jax.shard_map(body, mesh=split, in_specs=in_specs, out_specs=out_specs, check_vma=False)
```

```python
import functools
import math

import jax
import jax.numpy as jnp
from jax import lax
from jax.experimental import pallas as pl
from jax.experimental.pallas import tpu as pltpu
from jax.sharding import Mesh
from jax.sharding import PartitionSpec as P

NR = 2048
NC = 4096
ROW = ("row_0", "row_1")
COL = ("col_0", "col_1")
NEAR = ("row_1", "col_1")
FAR = ("row_0", "col_0")
SCALE = 1.0 / math.sqrt(NR * NC)
BEAMS, POOL, ROWS, LANES = 40, 12, 256, 128
GROUP = 8
LIMIT = 30 << 20
FIRST, CHUNK = 16, 4
EXACT = lax.Precision.HIGHEST
NN = (((1,), (0,)), ((), ()))
NT = (((1,), (1,)), ((), ()))
TN = (((0,), (0,)), ((), ()))
F32, BF16 = jnp.float32, jnp.bfloat16
VMEM = pl.BlockSpec(memory_space=pltpu.VMEM)
HBM = pl.BlockSpec(memory_space=pltpu.HBM)
SMEM = pl.BlockSpec(memory_space=pltpu.SMEM)


def iota(shape, dim):
    return lax.broadcasted_iota(jnp.int32, shape, dim)


def dot(a, b, dims, precision=None):
    return lax.dot_general(a, b, dims, precision=precision, preferred_element_type=F32)


def halves(x):
    high = x.astype(BF16)
    return high, (x - high.astype(F32)).astype(BF16)


def thirds(x):
    high = x.astype(BF16)
    rest = x - high.astype(F32)
    mid = rest.astype(BF16)
    return high, mid, (rest - mid.astype(F32)).astype(BF16)


def dot_exact(ones, x, dims):
    return sum(dot(ones.astype(BF16), part, dims) for part in thirds(x))


def exact_dot(x, ones, dims):
    return sum(dot(part, ones.astype(BF16), dims) for part in thirds(x))


def rows_around(x):
    zero = jnp.zeros((1, LANES), F32)
    return jnp.concatenate([x[1:], zero], axis=0) + jnp.concatenate([zero, x[:-1]], axis=0)


def band_matrix(center):
    away = jnp.abs(iota((LANES, LANES), 0) - iota((LANES, LANES), 1))
    return jnp.where(away == 0, center, jnp.where(away == 1, 1.0, 0.0))


def by_side(even, first, second):
    return jnp.where(even, second, first), jnp.where(even, first, second)


def line_ends(w_hbm, pool_hbm, first_ref, second_ref, w_buf, pool_buf, sems):
    copies = []
    for k, at in enumerate((0, ROWS - 8)):
        for j, (src, dst) in enumerate(((w_hbm, w_buf), (pool_hbm, pool_buf))):
            copies.append(pltpu.make_async_copy(src.at[:, at : at + 8, :], dst.at[k], sems.at[2 * k + j]))
    for copy in copies:
        copy.start()
    for copy in copies:
        copy.wait()
    even = lax.axis_index(ROW[1]) == 0
    for rows, buf, top, bottom in (
        (slice(0, 40), w_buf, 0, 7), (slice(40, 80), w_buf, 1, 6), (slice(80, 92), pool_buf, 0, 7)
    ):
        first_ref[rows, :], second_ref[rows, :] = by_side(even, buf[0, :, top, :], buf[1, :, bottom, :])
    for ref in (first_ref, second_ref):
        ref[92:96, :] = jnp.zeros((4, LANES), F32)


def column_ends(w_hbm, pool_hbm, first_ref, second_ref, w_buf, pool_buf, ends_ref, sems):
    copies = [pltpu.make_async_copy(pool_hbm, pool_buf, sems.at[5])]
    for k in range(5):
        copies.append(pltpu.make_async_copy(w_hbm.at[8 * k : 8 * k + 8], w_buf.at[8 * k : 8 * k + 8], sems.at[k]))
    for copy in copies[:2]:
        copy.start()
    row, lane = iota((8, LANES), 0), iota((8, LANES), 1)
    pick = jnp.zeros((8, LANES), F32)
    for k, spot in enumerate((0, LANES - 1, 1, LANES - 2)):
        pick = jnp.where((row == k) & (lane == spot), 1.0, pick)
    pick = pick.astype(BF16)
    pick = jnp.concatenate([pick, pick], axis=1)
    def image(p, carry):
        x = pool_buf[p]
        ends_ref[BEAMS + p] = dot(pick, jnp.concatenate(halves(x), axis=1), NT)
        return carry

    def beam(b, carry):
        ends_ref[b] = dot(pick, jnp.concatenate(halves(w_buf[b]), axis=1), NT)
        return carry

    for k, copy in enumerate(copies):
        copy.wait()
        if k == 0:
            copies[2].start()
            copies[3].start()
            lax.fori_loop(0, POOL, image, 0, unroll=4)
        else:
            if k + 3 < len(copies):
                copies[k + 3].start()
            lax.fori_loop(8 * k - 8, 8 * k, beam, 0, unroll=4)
    even = (lax.axis_index(COL[1]) & 1) == 0
    for rows, images, left, right in (
        (slice(0, 40), slice(0, 40), 0, 1), (slice(40, 80), slice(0, 40), 2, 3), (slice(80, 92), slice(40, 52), 0, 1)
    ):
        first_ref[rows, :], second_ref[rows, :] = by_side(even, ends_ref[images, left, :], ends_ref[images, right, :])
    for ref in (first_ref, second_ref):
        ref[92:96, :] = jnp.zeros((4, ROWS), F32)


def gram(w_ref, pool_ref, sums_ref, lap_hbm, acc_ref, lap_ref, sem):
    along = band_matrix(-4.0).astype(BF16)
    along = jnp.concatenate([along, along], axis=0)

    def image(p, carry):
        x = pool_ref[p]
        lap_ref[p] = rows_around(x) + dot(jnp.concatenate(halves(x), axis=1), along, NN)
        return carry

    lax.fori_loop(0, POOL, image, 0, unroll=4)
    keep = pltpu.make_async_copy(lap_ref, lap_hbm, sem)
    keep.start()
    acc_ref[...] = jnp.zeros_like(acc_ref)

    def pair(ref, count, t):
        parts = []
        for k in range(GROUP):
            at = pl.multiple_of(t * GROUP * 8 + k * 8, 8)
            parts.append(ref[:, pl.ds(at, 8), :].reshape(count * 8, LANES))
        return jnp.concatenate(parts, axis=1)

    def step(t, carry):
        p_high, p_low = halves(pair(pool_ref, POOL, t))
        l_high, l_low = halves(pair(lap_ref, POOL, t))
        w_high, w_low = halves(pair(w_ref, BEAMS, t))
        a_high = jnp.concatenate([w_high, p_high], axis=0)
        a_low = jnp.concatenate([w_low, p_low], axis=0)
        b_high = jnp.concatenate([p_high, l_high], axis=0)
        b_low = jnp.concatenate([p_low, l_low], axis=0)
        left = jnp.concatenate([a_high, a_high, a_low], axis=1)
        right = jnp.concatenate([b_high, b_low, b_high], axis=1)
        acc_ref[...] += dot(left, right, NT)
        return carry

    lax.fori_loop(0, 32 // GROUP, step, 0)
    n, m = acc_ref.shape
    same = (iota((n, m), 0) & 7) == (iota((n, m), 1) & 7)
    kept = jnp.where(same, acc_ref[...], 0.0)
    q, j = iota((32, m), 0), iota((32, m), 1) >> 3
    fold = jnp.where(((j < POOL) & (q == j)) | ((j >= POOL) & (q == j + 16 - POOL)), 1.0, 0.0)
    folded = dot_exact(fold, kept, NT)
    i, lane = iota((n, LANES), 0) >> 3, iota((n, LANES), 1)
    to_p = jnp.where(((i < BEAMS) & (lane == i)) | ((i >= BEAMS) & (lane == i + 80 - BEAMS)), 1.0, 0.0)
    to_l = jnp.where((i < BEAMS) & (lane == i + 40), 1.0, 0.0)
    sums = exact_dot(folded[0:16], to_p, NN) + exact_dot(folded[16:32], to_l, NN)
    sums_ref[...] = sums[0:POOL]
    keep.wait()


def cross(
    sums_ref, row_a, row_b, row_a_got, row_b_got, col_a, col_b, col_a_got, col_b_got, sent_ref
):
    even_row = lax.axis_index(ROW[1]) == 0
    even_col = (lax.axis_index(COL[1]) & 1) == 0
    halo, edge = [], []
    for even, got, own in ((even_col, (col_a_got, col_b_got), (col_a, col_b)), (even_row, (row_a_got, row_b_got), (row_a, row_b))):
        halo.extend(by_side(even, *[ref[80:96, :] for ref in got]))
        edge.extend(by_side(even, *[ref[0:40, :] for ref in own]))
    edge = jnp.concatenate(edge, axis=1)
    edge = jnp.concatenate([jnp.zeros((40, 768), F32), edge, jnp.zeros((48, 768), F32)], axis=0)
    sums = sums_ref[...] + dot(jnp.concatenate(halo, axis=1), edge, NT, EXACT)[0:POOL]
    flat = jnp.concatenate([sums[p : p + 1] for p in range(POOL)], axis=1)
    for k in range(16):
        sent_ref[k] = flat


def again(parts_ref, token_ref, out_ref):
    sums = parts_ref[0]
    for k in range(1, 16):
        sums = sums + parts_ref[k]
    for k in range(16):
        out_ref[k] = sums


def base(first, count, with_pool, smooth_ref, active_ref, w_hbm, lap_in_hbm, *rest):
    if with_pool:
        smooth_row_ref, active_row_ref, row_a, row_b, row_a_got, row_b_got, *rest = rest
        col_a, col_b, col_a_got, col_b_got, *rest = rest
        out_hbm, lap_hbm, fix_ref, slots_ref, turned_ref, *rest, lap_ref = rest
        top_ref, bottom_ref, up_ref, down_ref, left_ref, right_ref, west_ref, east_ref, w_ref, out_ref, sems = rest
    else:
        fix_ref, slots_ref, out_hbm, w_ref, out_ref, sems = rest
    parts = count // CHUNK
    loads, stores = [], []
    for k in range(parts):
        part = slice(CHUNK * k, CHUNK * (k + 1))
        source = w_hbm.at[first + CHUNK * k : first + CHUNK * (k + 1)]
        loads.append(pltpu.make_async_copy(source, w_ref.at[part], sems.at[0, k]))
        stores.append(pltpu.make_async_copy(out_ref.at[part], out_hbm.at[part], sems.at[1, k]))
    for copy in loads[:3]:
        copy.start()
    if with_pool:
        load_lap = pltpu.make_async_copy(lap_in_hbm, lap_ref, sems.at[0, parts])
        store_lap = pltpu.make_async_copy(lap_ref, lap_hbm, sems.at[1, parts])
        load_lap.start()
    if with_pool:
        even_row = lax.axis_index(ROW[1]) == 0
        even_col = (lax.axis_index(COL[1]) & 1) == 0
        top_ref[...], bottom_ref[...] = by_side(even_row, row_a[...], row_b[...])
        up_ref[...], down_ref[...] = by_side(even_row, row_a_got[...], row_b_got[...])
        left_ref[...], right_ref[...] = by_side(even_col, col_a[...], col_b[...])
        west_ref[...], east_ref[...] = by_side(even_col, col_a_got[...], col_b_got[...])
        for ref in (west_ref, east_ref):
            one, two = ref[96:136, 0:LANES], ref[96:136, LANES:]
            ref[96:136, 0:LANES], ref[96:136, LANES:] = by_side(even_row, one, two)
        def across(row):
            return jnp.broadcast_to(row, (8, BEAMS)).T[:, 0:1]

        smooth_row, active_row = smooth_row_ref[...], active_row_ref[...]
        live0 = jnp.where(active_row > 0, 1.0, 0.0)
        live1 = jnp.where(active_row > 1, 1.0, 0.0)
        a = across(smooth_row * (live0 + live1))
        c = across(smooth_row * smooth_row * live0 * live1)
        r = lax.axis_index(ROW[0]) * 2 + lax.axis_index(ROW[1])
        k = lax.axis_index(COL[0]) * 8 + lax.axis_index(COL[1])
        has_up, has_down = jnp.where(r > 0, 1.0, 0.0), jnp.where(r < 7, 1.0, 0.0)
        has_west, has_east = jnp.where(k > 0, 1.0, 0.0), jnp.where(k < 31, 1.0, 0.0)
        span, shifted, corner = slice(0, 40), slice(40, 80), slice(96, 136)
        wide, thin = iota((BEAMS, ROWS), 1), iota((BEAMS, LANES), 1)

        def mixed(near, far, own, prev, after):
            return a * near + c * (2.0 * (prev + after) - 8.0 * near + far + own), c * near

        def column(msg_ref, own_ref, far_ref, has):
            near = msg_ref[span, :] - far_ref[span, :]
            prev = jnp.where(wide == 0, 0.0, pltpu.roll(near, 1, 1))
            after = jnp.where(wide == ROWS - 1, 0.0, pltpu.roll(near, ROWS - 1, 1))
            far = msg_ref[shifted, :] - far_ref[shifted, :]
            return mixed(near, far, (has - 1.0) * own_ref[span, :], prev, after)

        def line(msg_ref, own_ref, far_ref, has, at):
            near = msg_ref[span, :] - far_ref[span, :]
            west = pltpu.roll(west_ref[corner, at : at + LANES] - far_ref[span, :], 1, 1)
            east = pltpu.roll(east_ref[corner, at : at + LANES] - far_ref[span, :], LANES - 1, 1)
            prev = jnp.where(thin == 0, west, pltpu.roll(near, 1, 1))
            after = jnp.where(thin == LANES - 1, east, pltpu.roll(near, LANES - 1, 1))
            far = msg_ref[shifted, :] - far_ref[shifted, :]
            return mixed(near, far, (has - 1.0) * own_ref[span, :], prev, after)

        fix_ref[...] = jnp.zeros_like(fix_ref)
        turned_ref[...] = jnp.zeros_like(turned_ref)

        def beams_at(k):
            return pl.ds(k, BEAMS, stride=4)

        def pools_at(k):
            return pl.ds(4 * BEAMS + k, POOL, stride=4)

        east, west = column(east_ref, right_ref, left_ref, has_east), column(west_ref, left_ref, right_ref, has_west)
        for k, (line_of, pool_of) in enumerate(
            ((east[1], None), (east[0], east_ref[80:92, :]), (west[0], west_ref[80:92, :]), (west[1], None))
        ):
            for h in range(2):
                part = slice(LANES * h, LANES * (h + 1))
                turned_ref[h, beams_at(k), :] = line_of[:, part]
                if pool_of is not None:
                    turned_ref[h, pools_at(k), :] = pool_of[:, part]
        for k in range(2):
            for h in range(2):
                part = slice(LANES * h, LANES * (h + 1))
                slots_ref[k, part, :] = turned_ref[h, LANES * k : LANES * (k + 1), :].T
        fix_ref[:, 0, 0:128], fix_ref[:, 1, 0:128] = line(up_ref, top_ref, bottom_ref, has_up, 0)
        fix_ref[:, 7, 128:256], fix_ref[:, 6, 128:256] = line(down_ref, bottom_ref, top_ref, has_down, LANES)
    lane = iota((ROWS, LANES), 1)
    at_edge = (lane < 2) | (lane >= LANES - 2)

    def placed(image):
        spun = pltpu.roll(slots_ref[image >> 5], (LANES - 2 - 4 * image) & (LANES - 1), 1)
        return jnp.where(at_edge, spun, 0.0)

    away = (iota((LANES, LANES), 0) - iota((LANES, LANES), 1)) & (LANES - 1)
    once = jnp.where(away == 0, -2.0, jnp.where((away == 1) | (away == LANES - 1), 1.0, 0.0))
    along = jnp.concatenate([once, dot(once, once, NN)], axis=1).astype(BF16)
    along = jnp.concatenate([along, along], axis=0)

    def around(x):
        return pltpu.roll(x, 1, 0) + pltpu.roll(x, ROWS - 1, 0)

    def beam(b, carry):
        s_b, n_b = smooth_ref[first + b], active_ref[first + b]
        r_0, r_1 = jnp.where(n_b > 0, s_b, 0.0), jnp.where(n_b > 1, s_b, 0.0)
        a_b, c_b = r_0 + r_1, r_0 * r_1
        x = w_ref[b]
        sides = dot(jnp.concatenate(halves(x), axis=1), along, NN)
        one, two = sides[:, :LANES], sides[:, LANES:]
        lines = around(x)
        inner = around((a_b - 2.0 * c_b) * x + (2.0 * c_b) * one + c_b * lines)
        kept = (1.0 - 2.0 * a_b + 4.0 * c_b) * x + (a_b - 4.0 * c_b) * one + c_b * two - (2.0 * c_b) * lines
        out = kept + inner + placed(first + b)
        out_ref[b, 8 : ROWS - 8, :] = out[8 : ROWS - 8]
        out_ref[b, 0:8, :] = out[0:8] + fix_ref[first + b, :, 0:128]
        out_ref[b, ROWS - 8 : ROWS, :] = out[ROWS - 8 :] + fix_ref[first + b, :, 128:256]
        return carry

    for k in range(parts):
        loads[k].wait()
        if k + 3 < parts:
            loads[k + 3].start()
        lax.fori_loop(CHUNK * k, CHUNK * (k + 1), beam, 0, unroll=4)
        stores[k].start()
        if k == 0 and with_pool:
            load_lap.wait()

            def pool_step(p, carry):
                lap_ref[p] = lap_ref[p] + placed(BEAMS + p)
                return carry

            lax.fori_loop(0, POOL, pool_step, 0, unroll=4)
            lap_ref[:, 0, :] += up_ref[80:92, :]
            lap_ref[:, ROWS - 1, :] += down_ref[80:92, :]
            store_lap.start()
    for store in stores:
        store.wait()
    if with_pool:
        store_lap.wait()


def finish(
    parts_ref, desired_ref, plan_ref, ref_ref, rate_ref, smooth_ref, active_ref, base_a_hbm, base_b_hbm, pool_hbm,
    lap_hbm, out_hbm, err_ref, base_ref, pool_ref, lap_ref, high_ref, low_ref, in_sems, out_sems,
):
    def rows_of(t):
        return pl.ds(pl.multiple_of(t * 32, 8), 32)

    def fetches(t):
        cut = base_a_hbm.shape[0]
        at = rows_of(t)
        pairs = (
            (base_a_hbm.at[:, at, :], base_ref.at[0:cut, at, :]),
            (base_b_hbm.at[:, at, :], base_ref.at[cut:BEAMS, at, :]),
            (pool_hbm.at[:, at, :], pool_ref.at[:, at, :]),
            (lap_hbm.at[:, at, :], lap_ref.at[:, at, :]),
        )
        return [pltpu.make_async_copy(src, dst, in_sems.at[k, t]) for k, (src, dst) in enumerate(pairs)]

    def store(t):
        at = rows_of(t)
        return pltpu.make_async_copy(base_ref.at[:, at, :], out_hbm.at[:, at, :], out_sems.at[t])

    for t in range(8):
        for copy in fetches(t):
            copy.start()

    sums = parts_ref[0]
    for k in range(1, 16):
        sums = sums + parts_ref[k]
    sums = jnp.concatenate([sums[:, LANES * p : LANES * (p + 1)] for p in range(POOL)], axis=0)
    one_hot = jnp.where(iota((8, BEAMS), 0) == ref_ref[...], 1.0, 0.0)
    target = dot(desired_ref[...], one_hot, TN, EXACT)
    rate, smooth = rate_ref[...] * SCALE, smooth_ref[...]
    live0 = jnp.where(active_ref[...] > 0, 1.0, 0.0)
    live1 = jnp.where(active_ref[...] > 1, 1.0, 0.0)
    hits = [jnp.where(iota((POOL, 16), 0) == plan_ref[t : t + 1, :], 1.0, 0.0) for t in range(2)]
    many = [jnp.sum(h, axis=1, keepdims=True) for h in hits]
    p0 = sums[:, 0:BEAMS]
    lap = pltpu.roll(sums, LANES - 40, 1)[:, 0:BEAMS]
    inner = pltpu.roll(sums, LANES - 80, 1)[:, 0:POOL]
    e0 = target - SCALE * p0
    c0 = many[0] * e0
    p1 = p0 + live0 * (rate * dot(inner, c0, NN, EXACT) + smooth * lap)
    e1 = target - SCALE * p1
    c1 = many[1] * e1
    d0 = rate * (live0 * c0 + live1 * c1)
    d1 = live0 * live1 * rate * smooth * c0
    gap = jnp.zeros((4, BEAMS), F32)
    both = jnp.concatenate([d0, gap, d1, gap], axis=0)
    spread = jnp.where((iota((320, BEAMS), 0) >> 3) == iota((320, BEAMS), 1), 1.0, 0.0)
    spread = spread.astype(BF16)
    q, j = iota((32, 192), 0), iota((32, 192), 1) >> 3
    fold = jnp.where(((j < POOL) & (q == j)) | ((j >= POOL) & (q == j + 16 - POOL)), 1.0, 0.0).astype(BF16)
    same = (iota((320, 192), 0) & 7) == (iota((320, 192), 1) & 7)
    for ref, part in zip((high_ref, low_ref), halves(both)):
        by_q = dot(spread, part, NT).astype(BF16)
        ref[...] = jnp.where(same, dot(by_q, fold, NN), 0.0).astype(BF16)

    def step(t, carry):
        for copy in fetches(t):
            copy.wait()

        def tile(ref, at):
            return ref.at[:, pl.ds(pl.multiple_of(t * 32 + at, 8), 8), :]

        for k in range(2):
            halves_of = []
            for h in range(2):
                at = 16 * k + 8 * h
                halves_of.append(
                    jnp.concatenate([tile(ref, at)[...].reshape(96, LANES) for ref in (pool_ref, lap_ref)], axis=0)
                )
            high, low = halves(jnp.concatenate(halves_of, axis=1))
            got = dot(high_ref[...], high, NN) + dot(high_ref[...], low, NN) + dot(low_ref[...], high, NN)
            for h in range(2):
                part = got[:, h * LANES : (h + 1) * LANES].reshape(BEAMS, 8, LANES)
                tile(base_ref, 16 * k + 8 * h)[...] += part
        store(t).start()
        return carry

    lax.fori_loop(0, 8, step, 0)
    for t, e in enumerate((e0, e1)):
        err_ref[t] = dot(hits[t], e, TN, EXACT)
    for t in range(8):
        store(t).wait()


def call(kernel, outs, specs, scratch=(), out_specs=None):
    run = pl.pallas_call(
        kernel,
        name=getattr(kernel, "__name__", "base"),
        out_shape=outs,
        in_specs=specs,
        out_specs=out_specs or [VMEM] * len(outs),
        scratch_shapes=scratch,
        compiler_params=pltpu.CompilerParams(vmem_limit_bytes=LIMIT),
    )
    homes = {id(VMEM): pltpu.VMEM, id(HBM): pltpu.HBM}

    def at_home(value, spec):
        return pltpu.with_memory_space_constraint(value, homes[id(spec)]) if id(spec) in homes else value

    return lambda *args: run(*[at_home(x, spec) for x, spec in zip(args, specs)])


def vmem(*dims):
    return pltpu.VMEM(dims, F32)


def far_out(*dims):
    return pltpu.HBM(dims, F32)


def swapped(value, axes, phase):
    count = lax.axis_size(axes)
    pairs = [(i, i + 1) for i in range(phase, count - 1, 2)]
    return lax.ppermute(value, axes, pairs + [(b, a) for a, b in pairs])


def exchange(value, axes):
    return lax.all_to_all(value, axes, split_axis=0, concat_axis=0, tiled=True)


def body(weights, pool, desired, plan, beam_ref, step_size, smoothing, active):
    DMA = pltpu.SemaphoreType.DMA
    row_a, row_b = call(
        line_ends,
        [vmem(96, LANES)] * 2,
        [HBM, HBM],
        [vmem(2, BEAMS, 8, LANES), vmem(2, POOL, 8, LANES), DMA((4,))],
    )(weights, pool)
    row_b_got = swapped(row_b, ROW, 1)
    row_a_got = swapped(row_a, ROW, 0)
    col_a, col_b, w_near, p_near = call(
        column_ends,
        [vmem(96, ROWS)] * 2 + [vmem(BEAMS, ROWS, LANES), vmem(POOL, ROWS, LANES)],
        [HBM, HBM],
        [vmem(BEAMS + POOL, 8, ROWS), DMA((6,))],
    )(weights, pool)
    corners = jnp.concatenate([row_a_got[0:40], row_b_got[0:40]], axis=1)
    col_a_got = swapped(jnp.concatenate([col_a, corners], axis=0), COL, 0)
    col_b_got = swapped(jnp.concatenate([col_b, corners], axis=0), COL, 1)
    sums, pool_lap = call(
        gram,
        [vmem(POOL, LANES), far_out(POOL, ROWS, LANES)],
        [VMEM] * 2,
        [vmem(416, 192), vmem(POOL, ROWS, LANES), DMA],
        [VMEM, HBM],
    )(w_near, p_near)
    edges = (row_a, row_b, row_a_got, row_b_got, col_a, col_b, col_a_got, col_b_got)
    (sent,) = call(cross, [vmem(16, 1, POOL * LANES)], [VMEM] * 9)(sums, *edges)
    near = exchange(sent, NEAR)
    rows = (smoothing[None, :], active[None, :])
    shared = (smoothing, active, weights, pool_lap, *rows, *edges)
    specs = [SMEM, SMEM, HBM, HBM] + [VMEM] * 10
    edge_scratch = (
        [vmem(2, 256, LANES)] + [vmem(96, LANES)] * 4 + [vmem(96, ROWS)] * 2 + [vmem(136, ROWS)] * 2
    )
    rest = BEAMS - FIRST
    based_a, lap, fix, slots = call(
        functools.partial(base, 0, FIRST, True),
        [
            far_out(FIRST, ROWS, LANES),
            far_out(POOL, ROWS, LANES),
            vmem(BEAMS, 8, 256),
            vmem(2, ROWS, LANES),
        ],
        specs,
        edge_scratch + [vmem(FIRST, ROWS, LANES)] * 2 + [DMA((2, FIRST // CHUNK + 1)), vmem(POOL, ROWS, LANES)],
        [HBM, HBM, VMEM, VMEM],
    )(*shared)
    (sent,) = call(again, [vmem(16, 1, POOL * LANES)], [VMEM] * 2)(near, slots)
    far = exchange(sent, FAR)
    (based_b,) = call(
        functools.partial(base, FIRST, rest, False),
        [far_out(rest, ROWS, LANES)],
        [SMEM, SMEM, HBM, HBM, VMEM, VMEM],
        [vmem(rest, ROWS, LANES)] * 2 + [DMA((2, rest // CHUNK))],
        [HBM],
    )(smoothing, active, weights, pool_lap, fix, slots)
    final, errors = call(
        finish,
        [far_out(BEAMS, ROWS, LANES), jax.ShapeDtypeStruct((2, 16, BEAMS), F32)],
        [VMEM] * 7 + [HBM] * 4,
        [
            vmem(BEAMS, ROWS, LANES),
            vmem(POOL, ROWS, LANES),
            vmem(POOL, ROWS, LANES),
            pltpu.VMEM((320, 192), BF16),
            pltpu.VMEM((320, 192), BF16),
            DMA((4, 8)),
            DMA((8,)),
        ],
        [HBM, VMEM],
    )(far, desired.T, plan, beam_ref[None, :], step_size[None, :], *rows, based_a, based_b, pool, lap)
    return final, jnp.swapaxes(errors, 1, 2)


def solution(mesh):
    split = Mesh(mesh.devices.reshape(4, 2, 4, 8), ("row_0", "row_1", "col_0", "col_1"))
    in_specs = (P(None, ROW, COL), P(None, ROW, COL), P(), P(), P(), P(), P(), P())
    out_specs = (P(None, ROW, COL), P())
    return jax.shard_map(body, mesh=split, in_specs=in_specs, out_specs=out_specs, check_vma=False)
```

```python
import functools
import math

import jax
import jax.numpy as jnp
from jax import lax
from jax.experimental import pallas as pl
from jax.experimental.pallas import tpu as pltpu
from jax.sharding import Mesh
from jax.sharding import PartitionSpec as P

NR = 2048
NC = 4096
ROW = ("row_0", "row_1")
COL = ("col_0", "col_1")
NEAR = ("row_1", "col_1")
FAR = ("row_0", "col_0")
SCALE = 1.0 / math.sqrt(NR * NC)
BEAMS, POOL, ROWS, LANES = 40, 12, 256, 128
GROUP = 8
LIMIT = 30 << 20
FIRST, CHUNK = 16, 4
EXACT = lax.Precision.HIGHEST
NN = (((1,), (0,)), ((), ()))
NT = (((1,), (1,)), ((), ()))
TN = (((0,), (0,)), ((), ()))
F32, BF16 = jnp.float32, jnp.bfloat16
VMEM = pl.BlockSpec(memory_space=pltpu.VMEM)
HBM = pl.BlockSpec(memory_space=pltpu.HBM)
SMEM = pl.BlockSpec(memory_space=pltpu.SMEM)


def iota(shape, dim):
    return lax.broadcasted_iota(jnp.int32, shape, dim)


def dot(a, b, dims, precision=None):
    return lax.dot_general(a, b, dims, precision=precision, preferred_element_type=F32)


def halves(x):
    high = x.astype(BF16)
    return high, (x - high.astype(F32)).astype(BF16)


def thirds(x):
    high = x.astype(BF16)
    rest = x - high.astype(F32)
    mid = rest.astype(BF16)
    return high, mid, (rest - mid.astype(F32)).astype(BF16)


def dot_exact(ones, x, dims):
    return sum(dot(ones.astype(BF16), part, dims) for part in thirds(x))


def exact_dot(x, ones, dims):
    return sum(dot(part, ones.astype(BF16), dims) for part in thirds(x))


def rows_around(x):
    zero = jnp.zeros((1, LANES), F32)
    return jnp.concatenate([x[1:], zero], axis=0) + jnp.concatenate([zero, x[:-1]], axis=0)


def band_matrix(center):
    away = jnp.abs(iota((LANES, LANES), 0) - iota((LANES, LANES), 1))
    return jnp.where(away == 0, center, jnp.where(away == 1, 1.0, 0.0))


def by_side(even, first, second):
    return jnp.where(even, second, first), jnp.where(even, first, second)


def line_ends(w_hbm, pool_hbm, first_ref, second_ref, w_buf, pool_buf, sems):
    copies = []
    for k, at in enumerate((0, ROWS - 8)):
        for j, (src, dst) in enumerate(((w_hbm, w_buf), (pool_hbm, pool_buf))):
            copies.append(pltpu.make_async_copy(src.at[:, at : at + 8, :], dst.at[k], sems.at[2 * k + j]))
    for copy in copies:
        copy.start()
    for copy in copies:
        copy.wait()
    even = lax.axis_index(ROW[1]) == 0
    for rows, buf, top, bottom in (
        (slice(0, 40), w_buf, 0, 7), (slice(40, 80), w_buf, 1, 6), (slice(80, 92), pool_buf, 0, 7)
    ):
        first_ref[rows, :], second_ref[rows, :] = by_side(even, buf[0, :, top, :], buf[1, :, bottom, :])
    for ref in (first_ref, second_ref):
        ref[92:96, :] = jnp.zeros((4, LANES), F32)


def column_ends(w_hbm, pool_hbm, first_ref, second_ref, w_buf, pool_buf, ends_ref, sems):
    copies = [pltpu.make_async_copy(pool_hbm, pool_buf, sems.at[5])]
    for k in range(5):
        copies.append(pltpu.make_async_copy(w_hbm.at[8 * k : 8 * k + 8], w_buf.at[8 * k : 8 * k + 8], sems.at[k]))
    for copy in copies[:2]:
        copy.start()
    row, lane = iota((8, LANES), 0), iota((8, LANES), 1)
    pick = jnp.zeros((8, LANES), F32)
    for k, spot in enumerate((0, LANES - 1, 1, LANES - 2)):
        pick = jnp.where((row == k) & (lane == spot), 1.0, pick)
    pick = pick.astype(BF16)
    pick = jnp.concatenate([pick, pick], axis=1)
    def image(p, carry):
        x = pool_buf[p]
        ends_ref[BEAMS + p] = dot(pick, jnp.concatenate(halves(x), axis=1), NT)
        return carry

    def beam(b, carry):
        ends_ref[b] = dot(pick, jnp.concatenate(halves(w_buf[b]), axis=1), NT)
        return carry

    for k, copy in enumerate(copies):
        copy.wait()
        if k == 0:
            copies[2].start()
            copies[3].start()
            lax.fori_loop(0, POOL, image, 0, unroll=4)
        else:
            if k + 3 < len(copies):
                copies[k + 3].start()
            lax.fori_loop(8 * k - 8, 8 * k, beam, 0, unroll=4)
    even = (lax.axis_index(COL[1]) & 1) == 0
    for rows, images, left, right in (
        (slice(0, 40), slice(0, 40), 0, 1), (slice(40, 80), slice(0, 40), 2, 3), (slice(80, 92), slice(40, 52), 0, 1)
    ):
        first_ref[rows, :], second_ref[rows, :] = by_side(even, ends_ref[images, left, :], ends_ref[images, right, :])
    for ref in (first_ref, second_ref):
        ref[92:96, :] = jnp.zeros((4, ROWS), F32)


def gram(w_ref, pool_ref, sums_ref, lap_hbm, acc_ref, lap_ref, sem):
    along = band_matrix(-4.0).astype(BF16)
    along = jnp.concatenate([along, along], axis=0)

    def image(p, carry):
        x = pool_ref[p]
        lap_ref[p] = rows_around(x) + dot(jnp.concatenate(halves(x), axis=1), along, NN)
        return carry

    lax.fori_loop(0, POOL, image, 0, unroll=4)
    keep = pltpu.make_async_copy(lap_ref, lap_hbm, sem)
    keep.start()
    acc_ref[...] = jnp.zeros_like(acc_ref)

    def pair(ref, count, t):
        parts = []
        for k in range(GROUP):
            at = pl.multiple_of(t * GROUP * 8 + k * 8, 8)
            parts.append(ref[:, pl.ds(at, 8), :].reshape(count * 8, LANES))
        return jnp.concatenate(parts, axis=1)

    def step(t, carry):
        p_high, p_low = halves(pair(pool_ref, POOL, t))
        l_high, l_low = halves(pair(lap_ref, POOL, t))
        w_high, w_low = halves(pair(w_ref, BEAMS, t))
        a_high = jnp.concatenate([w_high, p_high], axis=0)
        a_low = jnp.concatenate([w_low, p_low], axis=0)
        b_high = jnp.concatenate([p_high, l_high], axis=0)
        b_low = jnp.concatenate([p_low, l_low], axis=0)
        left = jnp.concatenate([a_high, a_high, a_low], axis=1)
        right = jnp.concatenate([b_high, b_low, b_high], axis=1)
        acc_ref[...] += dot(left, right, NT)
        return carry

    lax.fori_loop(0, 32 // GROUP, step, 0)
    n, m = acc_ref.shape
    same = (iota((n, m), 0) & 7) == (iota((n, m), 1) & 7)
    kept = jnp.where(same, acc_ref[...], 0.0)
    q, j = iota((32, m), 0), iota((32, m), 1) >> 3
    fold = jnp.where(((j < POOL) & (q == j)) | ((j >= POOL) & (q == j + 16 - POOL)), 1.0, 0.0)
    folded = dot_exact(fold, kept, NT)
    i, lane = iota((n, LANES), 0) >> 3, iota((n, LANES), 1)
    to_p = jnp.where(((i < BEAMS) & (lane == i)) | ((i >= BEAMS) & (lane == i + 80 - BEAMS)), 1.0, 0.0)
    to_l = jnp.where((i < BEAMS) & (lane == i + 40), 1.0, 0.0)
    sums = exact_dot(folded[0:16], to_p, NN) + exact_dot(folded[16:32], to_l, NN)
    sums_ref[...] = sums[0:POOL]
    keep.wait()


def cross(
    sums_ref, row_a, row_b, row_a_got, row_b_got, col_a, col_b, col_a_got, col_b_got, sent_ref
):
    even_row = lax.axis_index(ROW[1]) == 0
    even_col = (lax.axis_index(COL[1]) & 1) == 0
    halo, edge = [], []
    for even, got, own in ((even_col, (col_a_got, col_b_got), (col_a, col_b)), (even_row, (row_a_got, row_b_got), (row_a, row_b))):
        halo.extend(by_side(even, *[ref[80:96, :] for ref in got]))
        edge.extend(by_side(even, *[ref[0:40, :] for ref in own]))
    edge = jnp.concatenate(edge, axis=1)
    edge = jnp.concatenate([jnp.zeros((40, 768), F32), edge, jnp.zeros((48, 768), F32)], axis=0)
    sums = sums_ref[...] + dot(jnp.concatenate(halo, axis=1), edge, NT, EXACT)[0:POOL]
    flat = jnp.concatenate([sums[p : p + 1] for p in range(POOL)], axis=1)
    for k in range(16):
        sent_ref[k] = flat


def again(parts_ref, token_ref, out_ref):
    sums = parts_ref[0]
    for k in range(1, 16):
        sums = sums + parts_ref[k]
    for k in range(16):
        out_ref[k] = sums


def base(first, count, with_pool, smooth_ref, active_ref, w_hbm, lap_in_hbm, *rest):
    if with_pool:
        smooth_row_ref, active_row_ref, row_a, row_b, row_a_got, row_b_got, *rest = rest
        col_a, col_b, col_a_got, col_b_got, *rest = rest
        out_hbm, lap_hbm, fix_ref, slots_ref, turned_ref, *rest, lap_ref = rest
        top_ref, bottom_ref, up_ref, down_ref, left_ref, right_ref, west_ref, east_ref, w_ref, out_ref, sems = rest
    else:
        fix_ref, slots_ref, out_hbm, w_ref, out_ref, sems = rest
    parts = count // CHUNK
    loads, stores = [], []
    for k in range(parts):
        part = slice(CHUNK * k, CHUNK * (k + 1))
        source = w_hbm.at[first + CHUNK * k : first + CHUNK * (k + 1)]
        loads.append(pltpu.make_async_copy(source, w_ref.at[part], sems.at[0, k]))
        stores.append(pltpu.make_async_copy(out_ref.at[part], out_hbm.at[part], sems.at[1, k]))
    for copy in loads[:3]:
        copy.start()
    if with_pool:
        load_lap = pltpu.make_async_copy(lap_in_hbm, lap_ref, sems.at[0, parts])
        store_lap = pltpu.make_async_copy(lap_ref, lap_hbm, sems.at[1, parts])
        load_lap.start()
    if with_pool:
        even_row = lax.axis_index(ROW[1]) == 0
        even_col = (lax.axis_index(COL[1]) & 1) == 0
        top_ref[...], bottom_ref[...] = by_side(even_row, row_a[...], row_b[...])
        up_ref[...], down_ref[...] = by_side(even_row, row_a_got[...], row_b_got[...])
        left_ref[...], right_ref[...] = by_side(even_col, col_a[...], col_b[...])
        west_ref[...], east_ref[...] = by_side(even_col, col_a_got[...], col_b_got[...])
        for ref in (west_ref, east_ref):
            one, two = ref[96:136, 0:LANES], ref[96:136, LANES:]
            ref[96:136, 0:LANES], ref[96:136, LANES:] = by_side(even_row, one, two)
        def across(row):
            return jnp.broadcast_to(row, (8, BEAMS)).T[:, 0:1]

        smooth_row, active_row = smooth_row_ref[...], active_row_ref[...]
        live0 = jnp.where(active_row > 0, 1.0, 0.0)
        live1 = jnp.where(active_row > 1, 1.0, 0.0)
        a = across(smooth_row * (live0 + live1))
        c = across(smooth_row * smooth_row * live0 * live1)
        r = lax.axis_index(ROW[0]) * 2 + lax.axis_index(ROW[1])
        k = lax.axis_index(COL[0]) * 8 + lax.axis_index(COL[1])
        has_up, has_down = jnp.where(r > 0, 1.0, 0.0), jnp.where(r < 7, 1.0, 0.0)
        has_west, has_east = jnp.where(k > 0, 1.0, 0.0), jnp.where(k < 31, 1.0, 0.0)
        span, shifted, corner = slice(0, 40), slice(40, 80), slice(96, 136)
        wide, thin = iota((BEAMS, ROWS), 1), iota((BEAMS, LANES), 1)

        def mixed(near, far, own, prev, after):
            return a * near + c * (2.0 * (prev + after) - 8.0 * near + far + own), c * near

        def column(msg_ref, own_ref, far_ref, has):
            near = msg_ref[span, :] - far_ref[span, :]
            prev = jnp.where(wide == 0, 0.0, pltpu.roll(near, 1, 1))
            after = jnp.where(wide == ROWS - 1, 0.0, pltpu.roll(near, ROWS - 1, 1))
            far = msg_ref[shifted, :] - far_ref[shifted, :]
            return mixed(near, far, (has - 1.0) * own_ref[span, :], prev, after)

        def line(msg_ref, own_ref, far_ref, has, at):
            near = msg_ref[span, :] - far_ref[span, :]
            west = pltpu.roll(west_ref[corner, at : at + LANES] - far_ref[span, :], 1, 1)
            east = pltpu.roll(east_ref[corner, at : at + LANES] - far_ref[span, :], LANES - 1, 1)
            prev = jnp.where(thin == 0, west, pltpu.roll(near, 1, 1))
            after = jnp.where(thin == LANES - 1, east, pltpu.roll(near, LANES - 1, 1))
            far = msg_ref[shifted, :] - far_ref[shifted, :]
            return mixed(near, far, (has - 1.0) * own_ref[span, :], prev, after)

        fix_ref[...] = jnp.zeros_like(fix_ref)
        turned_ref[...] = jnp.zeros_like(turned_ref)

        def beams_at(k):
            return pl.ds(k, BEAMS, stride=4)

        def pools_at(k):
            return pl.ds(4 * BEAMS + k, POOL, stride=4)

        east, west = column(east_ref, right_ref, left_ref, has_east), column(west_ref, left_ref, right_ref, has_west)
        for k, (line_of, pool_of) in enumerate(
            ((east[1], None), (east[0], east_ref[80:92, :]), (west[0], west_ref[80:92, :]), (west[1], None))
        ):
            for h in range(2):
                part = slice(LANES * h, LANES * (h + 1))
                turned_ref[h, beams_at(k), :] = line_of[:, part]
                if pool_of is not None:
                    turned_ref[h, pools_at(k), :] = pool_of[:, part]
        for k in range(2):
            for h in range(2):
                part = slice(LANES * h, LANES * (h + 1))
                slots_ref[k, part, :] = turned_ref[h, LANES * k : LANES * (k + 1), :].T
        fix_ref[:, 0, 0:128], fix_ref[:, 1, 0:128] = line(up_ref, top_ref, bottom_ref, has_up, 0)
        fix_ref[:, 7, 128:256], fix_ref[:, 6, 128:256] = line(down_ref, bottom_ref, top_ref, has_down, LANES)
    lane = iota((ROWS, LANES), 1)
    at_edge = (lane < 2) | (lane >= LANES - 2)

    def placed(image):
        spun = pltpu.roll(slots_ref[image >> 5], (LANES - 2 - 4 * image) & (LANES - 1), 1)
        return jnp.where(at_edge, spun, 0.0)

    away = (iota((LANES, LANES), 0) - iota((LANES, LANES), 1)) & (LANES - 1)
    once = jnp.where(away == 0, -2.0, jnp.where((away == 1) | (away == LANES - 1), 1.0, 0.0))
    along = jnp.concatenate([once, dot(once, once, NN)], axis=1).astype(BF16)
    along = jnp.concatenate([along, along], axis=0)

    def around(x):
        return pltpu.roll(x, 1, 0) + pltpu.roll(x, ROWS - 1, 0)

    def beam(b, carry):
        s_b, n_b = smooth_ref[first + b], active_ref[first + b]
        r_0, r_1 = jnp.where(n_b > 0, s_b, 0.0), jnp.where(n_b > 1, s_b, 0.0)
        a_b, c_b = r_0 + r_1, r_0 * r_1
        x = w_ref[b]
        sides = dot(jnp.concatenate(halves(x), axis=1), along, NN)
        one, two = sides[:, :LANES], sides[:, LANES:]
        lines = around(x)
        inner = around((a_b - 2.0 * c_b) * x + (2.0 * c_b) * one + c_b * lines)
        kept = (1.0 - 2.0 * a_b + 4.0 * c_b) * x + (a_b - 4.0 * c_b) * one + c_b * two - (2.0 * c_b) * lines
        out = kept + inner + placed(first + b)
        out_ref[b, 8 : ROWS - 8, :] = out[8 : ROWS - 8]
        out_ref[b, 0:8, :] = out[0:8] + fix_ref[first + b, :, 0:128]
        out_ref[b, ROWS - 8 : ROWS, :] = out[ROWS - 8 :] + fix_ref[first + b, :, 128:256]
        return carry

    for k in range(parts):
        loads[k].wait()
        if k + 3 < parts:
            loads[k + 3].start()
        lax.fori_loop(CHUNK * k, CHUNK * (k + 1), beam, 0, unroll=4)
        stores[k].start()
        if k == 0 and with_pool:
            load_lap.wait()

            def pool_step(p, carry):
                lap_ref[p] = lap_ref[p] + placed(BEAMS + p)
                return carry

            lax.fori_loop(0, POOL, pool_step, 0, unroll=4)
            lap_ref[:, 0, :] += up_ref[80:92, :]
            lap_ref[:, ROWS - 1, :] += down_ref[80:92, :]
            store_lap.start()
    for store in stores:
        store.wait()
    if with_pool:
        store_lap.wait()


def finish(
    parts_ref, desired_ref, plan_ref, ref_ref, rate_ref, smooth_ref, active_ref, base_a_hbm, base_b_hbm, pool_hbm,
    lap_hbm, out_hbm, err_ref, base_ref, pool_ref, lap_ref, high_ref, low_ref, in_sems, out_sems,
):
    def rows_of(t):
        return pl.ds(pl.multiple_of(t * 32, 8), 32)

    def fetches(t):
        cut = base_a_hbm.shape[0]
        at = rows_of(t)
        pairs = (
            (base_a_hbm.at[:, at, :], base_ref.at[0:cut, at, :]),
            (base_b_hbm.at[:, at, :], base_ref.at[cut:BEAMS, at, :]),
            (pool_hbm.at[:, at, :], pool_ref.at[:, at, :]),
            (lap_hbm.at[:, at, :], lap_ref.at[:, at, :]),
        )
        return [pltpu.make_async_copy(src, dst, in_sems.at[k, t]) for k, (src, dst) in enumerate(pairs)]

    def store(t):
        at = rows_of(t)
        return pltpu.make_async_copy(base_ref.at[:, at, :], out_hbm.at[:, at, :], out_sems.at[t])

    for t in range(8):
        for copy in fetches(t):
            copy.start()

    sums = parts_ref[0]
    for k in range(1, 16):
        sums = sums + parts_ref[k]
    sums = jnp.concatenate([sums[:, LANES * p : LANES * (p + 1)] for p in range(POOL)], axis=0)
    one_hot = jnp.where(iota((8, BEAMS), 0) == ref_ref[...], 1.0, 0.0)
    target = dot(desired_ref[...], one_hot, TN, EXACT)
    rate, smooth = rate_ref[...] * SCALE, smooth_ref[...]
    live0 = jnp.where(active_ref[...] > 0, 1.0, 0.0)
    live1 = jnp.where(active_ref[...] > 1, 1.0, 0.0)
    hits = [jnp.where(iota((POOL, 16), 0) == plan_ref[t : t + 1, :], 1.0, 0.0) for t in range(2)]
    many = [jnp.sum(h, axis=1, keepdims=True) for h in hits]
    p0 = sums[:, 0:BEAMS]
    lap = pltpu.roll(sums, LANES - 40, 1)[:, 0:BEAMS]
    inner = pltpu.roll(sums, LANES - 80, 1)[:, 0:POOL]
    e0 = target - SCALE * p0
    c0 = many[0] * e0
    p1 = p0 + live0 * (rate * dot(inner, c0, NN, EXACT) + smooth * lap)
    e1 = target - SCALE * p1
    c1 = many[1] * e1
    d0 = rate * (live0 * c0 + live1 * c1)
    d1 = live0 * live1 * rate * smooth * c0
    gap = jnp.zeros((4, BEAMS), F32)
    both = jnp.concatenate([d0, gap, d1, gap], axis=0)
    spread = jnp.where((iota((320, BEAMS), 0) >> 3) == iota((320, BEAMS), 1), 1.0, 0.0)
    spread = spread.astype(BF16)
    q, j = iota((32, 192), 0), iota((32, 192), 1) >> 3
    fold = jnp.where(((j < POOL) & (q == j)) | ((j >= POOL) & (q == j + 16 - POOL)), 1.0, 0.0).astype(BF16)
    same = (iota((320, 192), 0) & 7) == (iota((320, 192), 1) & 7)
    for ref, part in zip((high_ref, low_ref), halves(both)):
        by_q = dot(spread, part, NT).astype(BF16)
        ref[...] = jnp.where(same, dot(by_q, fold, NN), 0.0).astype(BF16)

    def step(t, carry):
        for copy in fetches(t):
            copy.wait()

        def tile(ref, at):
            return ref.at[:, pl.ds(pl.multiple_of(t * 32 + at, 8), 8), :]

        for k in range(2):
            halves_of = []
            for h in range(2):
                at = 16 * k + 8 * h
                halves_of.append(
                    jnp.concatenate([tile(ref, at)[...].reshape(96, LANES) for ref in (pool_ref, lap_ref)], axis=0)
                )
            high, low = halves(jnp.concatenate(halves_of, axis=1))
            got = dot(high_ref[...], high, NN) + dot(high_ref[...], low, NN) + dot(low_ref[...], high, NN)
            for h in range(2):
                part = got[:, h * LANES : (h + 1) * LANES].reshape(BEAMS, 8, LANES)
                tile(base_ref, 16 * k + 8 * h)[...] += part
        store(t).start()
        return carry

    lax.fori_loop(0, 8, step, 0, unroll=2)
    for t, e in enumerate((e0, e1)):
        err_ref[t] = dot(hits[t], e, TN, EXACT)
    for t in range(8):
        store(t).wait()


def call(kernel, outs, specs, scratch=(), out_specs=None):
    run = pl.pallas_call(
        kernel,
        name=getattr(kernel, "__name__", "base"),
        out_shape=outs,
        in_specs=specs,
        out_specs=out_specs or [VMEM] * len(outs),
        scratch_shapes=scratch,
        compiler_params=pltpu.CompilerParams(vmem_limit_bytes=LIMIT),
    )
    homes = {id(VMEM): pltpu.VMEM, id(HBM): pltpu.HBM}

    def at_home(value, spec):
        return pltpu.with_memory_space_constraint(value, homes[id(spec)]) if id(spec) in homes else value

    return lambda *args: run(*[at_home(x, spec) for x, spec in zip(args, specs)])


def vmem(*dims):
    return pltpu.VMEM(dims, F32)


def far_out(*dims):
    return pltpu.HBM(dims, F32)


def swapped(value, axes, phase):
    count = lax.axis_size(axes)
    pairs = [(i, i + 1) for i in range(phase, count - 1, 2)]
    return lax.ppermute(value, axes, pairs + [(b, a) for a, b in pairs])


def exchange(value, axes):
    return lax.all_to_all(value, axes, split_axis=0, concat_axis=0, tiled=True)


def body(weights, pool, desired, plan, beam_ref, step_size, smoothing, active):
    DMA = pltpu.SemaphoreType.DMA
    row_a, row_b = call(
        line_ends,
        [vmem(96, LANES)] * 2,
        [HBM, HBM],
        [vmem(2, BEAMS, 8, LANES), vmem(2, POOL, 8, LANES), DMA((4,))],
    )(weights, pool)
    row_b_got = swapped(row_b, ROW, 1)
    row_a_got = swapped(row_a, ROW, 0)
    col_a, col_b, w_near, p_near = call(
        column_ends,
        [vmem(96, ROWS)] * 2 + [vmem(BEAMS, ROWS, LANES), vmem(POOL, ROWS, LANES)],
        [HBM, HBM],
        [vmem(BEAMS + POOL, 8, ROWS), DMA((6,))],
    )(weights, pool)
    corners = jnp.concatenate([row_a_got[0:40], row_b_got[0:40]], axis=1)
    col_a_got = swapped(jnp.concatenate([col_a, corners], axis=0), COL, 0)
    col_b_got = swapped(jnp.concatenate([col_b, corners], axis=0), COL, 1)
    sums, pool_lap = call(
        gram,
        [vmem(POOL, LANES), far_out(POOL, ROWS, LANES)],
        [VMEM] * 2,
        [vmem(416, 192), vmem(POOL, ROWS, LANES), DMA],
        [VMEM, HBM],
    )(w_near, p_near)
    edges = (row_a, row_b, row_a_got, row_b_got, col_a, col_b, col_a_got, col_b_got)
    (sent,) = call(cross, [vmem(16, 1, POOL * LANES)], [VMEM] * 9)(sums, *edges)
    near = exchange(sent, NEAR)
    rows = (smoothing[None, :], active[None, :])
    shared = (smoothing, active, weights, pool_lap, *rows, *edges)
    specs = [SMEM, SMEM, HBM, HBM] + [VMEM] * 10
    edge_scratch = (
        [vmem(2, 256, LANES)] + [vmem(96, LANES)] * 4 + [vmem(96, ROWS)] * 2 + [vmem(136, ROWS)] * 2
    )
    rest = BEAMS - FIRST
    based_a, lap, fix, slots = call(
        functools.partial(base, 0, FIRST, True),
        [
            far_out(FIRST, ROWS, LANES),
            far_out(POOL, ROWS, LANES),
            vmem(BEAMS, 8, 256),
            vmem(2, ROWS, LANES),
        ],
        specs,
        edge_scratch + [vmem(FIRST, ROWS, LANES)] * 2 + [DMA((2, FIRST // CHUNK + 1)), vmem(POOL, ROWS, LANES)],
        [HBM, HBM, VMEM, VMEM],
    )(*shared)
    (sent,) = call(again, [vmem(16, 1, POOL * LANES)], [VMEM] * 2)(near, slots)
    far = exchange(sent, FAR)
    (based_b,) = call(
        functools.partial(base, FIRST, rest, False),
        [far_out(rest, ROWS, LANES)],
        [SMEM, SMEM, HBM, HBM, VMEM, VMEM],
        [vmem(rest, ROWS, LANES)] * 2 + [DMA((2, rest // CHUNK))],
        [HBM],
    )(smoothing, active, weights, pool_lap, fix, slots)
    final, errors = call(
        finish,
        [far_out(BEAMS, ROWS, LANES), jax.ShapeDtypeStruct((2, 16, BEAMS), F32)],
        [VMEM] * 7 + [HBM] * 4,
        [
            vmem(BEAMS, ROWS, LANES),
            vmem(POOL, ROWS, LANES),
            vmem(POOL, ROWS, LANES),
            pltpu.VMEM((320, 192), BF16),
            pltpu.VMEM((320, 192), BF16),
            DMA((4, 8)),
            DMA((8,)),
        ],
        [HBM, VMEM],
    )(far, desired.T, plan, beam_ref[None, :], step_size[None, :], *rows, based_a, based_b, pool, lap)
    return final, jnp.swapaxes(errors, 1, 2)


def solution(mesh):
    split = Mesh(mesh.devices.reshape(4, 2, 4, 8), ("row_0", "row_1", "col_0", "col_1"))
    in_specs = (P(None, ROW, COL), P(None, ROW, COL), P(), P(), P(), P(), P(), P())
    out_specs = (P(None, ROW, COL), P())
    return jax.shard_map(body, mesh=split, in_specs=in_specs, out_specs=out_specs, check_vma=False)
```
